32 devices in a mesh: grp: 8 (over z, x), tbl: 4 (over y, core).
Axes of the slice: x: 2, y: 2, z: 4, core: 2. Of those that a mesh axis runs over, the one named last changes fastest.
Arguments:
- next_ids: int32 [4096, 224], P(('grp', 'tbl')), may hold values from 0 to 6143
- next_lengths: int32 [4096, 26], P(('grp', 'tbl')), may hold values from 1 to 8
- slot_of_table: int32 [26], replicated, may hold values from 0 to 27, as said below
- tables: bfloat16 [28, 6144, 128], P('tbl'), may hold values from -2.5 to 2.5
- cross_input: bfloat16 [4096, 3456], P(('grp', 'tbl')), may hold values from -6 to 6
- cotangent: bfloat16 [4096, 3456], P(('grp', 'tbl')), may hold values from -6 to 6
- up_weight: bfloat16 [256, 3456], replicated, may hold values from -0.375 to 0.375
- down_weight: bfloat16 [3456, 256], replicated, may hold values from -0.109375 to 0.109375
Outputs:
- next_embedded: bfloat16 [4096, 3328], P(('grp', 'tbl'))
- grad_up: float32 [256, 3456], P('tbl', 'grp')
- grad_down: float32 [3456, 256], P('grp', 'tbl')
The draws below stay inside these ranges and needn't reach their ends.
Inputs may be any that keep to these rules, and one draw needn't show every extreme that they name: `next_ids`: entry 8 * s + k of an example's row is the k-th id of the bag held in slot s; entries with k at or past the bag's length, and all entries of slots that hold no table, are padding. `slot_of_table`: distinct slots; owner o along tbl holds slots o * 7 to o * 7 + 6, so an owner holds up to 7 tables and some owner holds exactly 7.
All inputs are finite; a program needn't handle non-finite values.
Results may differ from the reference program's by a relative error of at most 0.0049.
Values may be sent and summed in bfloat16 or wider, within the bound.
A program may use at most 128 MiB of HBM per device.

```python
import math
import jax
import jax.numpy as jnp
import numpy as np
from jax import lax

F = 26
E = 128
R = 256
MAXLEN = 8
ROWS = 6144
B_DEV = 128
D = 3456
TOKENS = 4096
SLOTS_ALL = 28
N_TBL = 4


def draw_slot_of_table(key, part):
    return jax.random.permutation(key, SLOTS_ALL)[:F].astype(jnp.int32)


def plant(entries, stream_key, smallest, top_value):
    shape = entries.shape
    place = [jax.random.randint(jax.random.fold_in(stream_key, axis), (), 0, shape[axis]) for axis in range(len(shape))]
    entries = entries.at[tuple(place)].set(smallest)
    longest = shape.index(max(shape))
    place[longest] = (place[longest] + 1) % shape[longest]
    return entries.at[tuple(place)].set(top_value)


def block_scale(stream_key, shape, split, low, largest):
    loudness, own = 1.0, jax.random.fold_in(stream_key, 6)
    for dim, shards_of in split:
        heights = jnp.exp(jax.random.uniform(jax.random.fold_in(own, dim), (shards_of,), jnp.float32, low / len(split), largest / len(split)))
        loudness = loudness * jnp.repeat(heights, shape[dim] // shards_of).reshape([-1 if axis == dim else 1 for axis in range(len(shape))])
    return loudness


def cumulative_ranks(amount, slope):
    loads = [(1 << 20) // math.isqrt(standing ** slope) + 1 for standing in range(1, amount + 1)]
    deviation = 1 + sum(loads) // (1 << 30)
    return np.cumsum(np.array([max(1, weight // deviation) for weight in loads]))


def ranked_ids(key, extent, number_of, lean):
    table = cumulative_ranks(number_of, lean)
    pick = jax.random.randint(jax.random.fold_in(key, 1), extent, 0, int(table[number_of - 1]))
    grade = jnp.searchsorted(jnp.asarray(table, jnp.int32), pick, side="right")
    return jax.random.permutation(jax.random.fold_in(key, 2), number_of)[grade].astype(jnp.int32)


def gaussian(rng, extent, width, most, cuts=(), kind=jnp.bfloat16):
    entries = jax.random.normal(rng, extent, jnp.float32) * width
    if len(cuts) > 0:
        entries = block_scale(rng, extent, cuts, -0.22, 0.18) * entries
    return jnp.clip(entries, min=-most, max=most).astype(kind)


def setup_inputs(seed: int = 0) -> dict:
    key_list = jax.random.split(jax.random.key(seed), 9)
    return {
        "next_ids": plant(ranked_ids(key_list[0], (TOKENS, SLOTS_ALL * MAXLEN), ROWS, 2), jax.random.fold_in(key_list[0], 3), 0, ROWS - 1).astype(jnp.int32),
        "next_lengths": plant(jax.random.randint(key_list[1], (TOKENS, F), 1, MAXLEN + 1), jax.random.fold_in(key_list[1], 1), 1, MAXLEN).astype(jnp.int32),
        "slot_of_table": draw_slot_of_table(jax.random.fold_in(key_list[8], 71), 0),
        "tables": gaussian(key_list[3], (SLOTS_ALL, ROWS, E), 0.35, 2.5, ((0, 4),)),
        "cross_input": gaussian(key_list[4], (TOKENS, D), 1.0, 6.0, ((0, 32),)),
        "cotangent": gaussian(key_list[5], (TOKENS, D), 1.0, 6.0, ((0, 32),)),
        "up_weight": gaussian(key_list[6], (R, D), R ** -0.5, 0.375),
        "down_weight": gaussian(key_list[7], (D, R), D ** -0.5, 0.109375),
    }


def pool_block(tables, slot_of_table, ids, lengths):
    count = ids.shape[0]
    ids_three = ids.reshape(count, SLOTS_ALL, MAXLEN)
    chosen = jnp.take(ids_three, slot_of_table, axis=1)
    flat_table = tables.reshape(SLOTS_ALL * ROWS, E)
    index = (chosen + (slot_of_table * ROWS)[None, :, None]).astype(jnp.int32)
    picked = jnp.take(flat_table, index.reshape(-1), axis=0).reshape(count, F, MAXLEN, E)
    keep = lax.broadcasted_iota(jnp.int32, (count, F, MAXLEN), 2) < lengths[:, :, None]
    masked = jnp.where(keep[..., None], picked, jnp.zeros((), picked.dtype))
    pooled = lax.optimization_barrier(jnp.sum(masked.astype(jnp.float32), axis=2))
    return pooled.astype(jnp.bfloat16).reshape(count, F * E)

def reference(next_ids, next_lengths, slot_of_table, tables, cross_input, cotangent, up_weight, down_weight):
    blocks = TOKENS // B_DEV
    id_blocks = next_ids.reshape(blocks, B_DEV, SLOTS_ALL * MAXLEN)
    len_blocks = next_lengths.reshape(blocks, B_DEV, F)
    pooled = lax.map(lambda pair: pool_block(tables, slot_of_table, pair[0], pair[1]), (id_blocks, len_blocks))
    next_embedded = pooled.reshape(TOKENS, F * E)
    span = B_DEV * N_TBL
    input_blocks = cross_input.reshape(TOKENS // span, span, D)
    grad_blocks = cotangent.reshape(TOKENS // span, span, D)

    def step(carry, pair):
        total_up, total_down = carry
        inputs, grads = pair
        low = jnp.dot(inputs, down_weight, preferred_element_type=jnp.float32).astype(jnp.bfloat16)
        dz = (grads.astype(jnp.float32) * inputs.astype(jnp.float32)).astype(jnp.bfloat16)
        dlow = jnp.dot(dz, up_weight.T, preferred_element_type=jnp.float32).astype(jnp.bfloat16)
        total_up = total_up + jnp.dot(low.T, dz, preferred_element_type=jnp.float32)
        total_down = total_down + jnp.dot(inputs.T, dlow, preferred_element_type=jnp.float32)
        return ((total_up, total_down), None)
    start = (jnp.zeros((R, D), jnp.float32), jnp.zeros((D, R), jnp.float32))
    (total_up, total_down), unused = lax.scan(step, start, (input_blocks, grad_blocks))
    factor = 1.0 / math.sqrt(TOKENS)
    return (next_embedded, total_up * factor, total_down * factor)
```

```python
import functools
import math

import jax
import jax.numpy as jnp
from jax import lax
from jax.experimental import pallas as pl
from jax.experimental.pallas import tpu as pltpu
from jax.sharding import PartitionSpec as P

LANES = 128


def pool_kernel(maxlen, idx_ref, tab_ref, out_ref, stage, wide, acc, sem):
    owners, batch, _ = out_ref.shape
    slots, rows, width = tab_ref.shape
    per_line = LANES // maxlen
    lines = batch // per_line
    chunk = 256

    def fetch(s):
        return pltpu.make_async_copy(tab_ref.at[s], stage.at[s % 2], sem.at[s % 2])

    fetch(0).start()
    wide[pl.ds(rows, 8), :] = jnp.zeros((8, width), jnp.float32)
    for s in range(slots):
        if s + 1 < slots:
            fetch(s + 1).start()
        fetch(s).wait()

        @pl.loop(0, rows // chunk)
        def _(c):
            at = pl.ds(pl.multiple_of(c * chunk, chunk), chunk)
            wide[at, :] = stage[s % 2, at, :].astype(jnp.float32)

        @pl.loop(0, owners * lines)
        def _(g):
            src = g // lines
            line = s * lines + g % lines
            for u in range(per_line):
                got = [
                    wide[pl.ds(idx_ref[src, line, u * maxlen + k], 1), :] for k in range(maxlen)
                ]
                while len(got) > 1:
                    got = [a + b for a, b in zip(got[::2], got[1::2])] + (
                        [got[-1]] if len(got) % 2 else []
                    )
                acc[pl.ds(g * per_line + u, 1), :] = got[0]

        for o in range(owners):
            out_ref[o, :, s * width : (s + 1) * width] = acc[
                o * batch : (o + 1) * batch, :
            ].astype(jnp.bfloat16)


def pool(idx, tables, batch, maxlen):
    slots, rows, width = tables.shape
    owners = idx.shape[0]
    return pl.pallas_call(
        functools.partial(pool_kernel, maxlen),
        out_shape=jax.ShapeDtypeStruct((owners, batch, slots * width), jnp.bfloat16),
        in_specs=[
            pl.BlockSpec(memory_space=pltpu.SMEM),
            pl.BlockSpec(memory_space=pl.ANY),
        ],
        out_specs=pl.BlockSpec(memory_space=pltpu.VMEM),
        scratch_shapes=[
            pltpu.VMEM((2, rows, width), jnp.bfloat16),
            pltpu.VMEM((rows + 8, width), jnp.float32),
            pltpu.VMEM((owners * batch, width), jnp.float32),
            pltpu.SemaphoreType.DMA((2,)),
        ],
        compiler_params=pltpu.CompilerParams(vmem_limit_bytes=60 << 20),
        cost_estimate=pl.CostEstimate(
            flops=100_000_000, bytes_accessed=tables.size * 2, transcendentals=0
        ),
        name="pool",
    )(idx, tables)


def order_kernel(slot_ref, got_ref, out_ref):
    owners, batch, wide = got_ref.shape
    feats = slot_ref.shape[0]
    width = out_ref.shape[1] // feats
    slots = wide // width
    for f in range(feats):
        s = slot_ref[f]
        at = pl.ds(pl.multiple_of(lax.rem(s, slots) * width, width), width)
        out_ref[:, f * width : (f + 1) * width] = got_ref[lax.div(s, slots), :, at]


def order(slot_of_table, got, width):
    return pl.pallas_call(
        order_kernel,
        out_shape=jax.ShapeDtypeStruct(
            (got.shape[1], slot_of_table.shape[0] * width), jnp.bfloat16
        ),
        in_specs=[
            pl.BlockSpec(memory_space=pltpu.SMEM),
            pl.BlockSpec(memory_space=pltpu.VMEM),
        ],
        out_specs=pl.BlockSpec(memory_space=pltpu.VMEM),
        name="order",
    )(slot_of_table, got)


def bag_rows(next_ids, next_lengths, slot_of_table, slots, owners, rows):
    batch = next_ids.shape[0]
    slots_all = slots * owners
    maxlen = next_ids.shape[1] // slots_all
    hit = (slot_of_table[:, None] == lax.broadcasted_iota(jnp.int32, (1, slots_all), 1)).astype(
        jnp.int32
    )
    slot_lengths = jnp.sum(next_lengths[:, :, None] * hit[None, :, :], axis=1)
    keep = lax.broadcasted_iota(jnp.int32, (batch, slots_all, maxlen), 2) < slot_lengths[:, :, None]
    idx = jnp.where(keep, next_ids.reshape(batch, slots_all, maxlen), rows)
    return idx.transpose(1, 0, 2).reshape(owners, slots * batch * maxlen // LANES, LANES)


def plain(
    next_ids, next_lengths, slot_of_table, tables, cross_input, cotangent, up_weight, down_weight
):
    batch = next_ids.shape[0]
    owners = lax.axis_size("tbl")
    slots, rows, width = tables.shape
    maxlen = next_ids.shape[1] // (slots * owners)
    idx = bag_rows(next_ids, next_lengths, slot_of_table, slots, owners, rows)
    low = jnp.dot(cross_input, down_weight, preferred_element_type=jnp.float32).astype(jnp.bfloat16)
    dz = (cotangent.astype(jnp.float32) * cross_input.astype(jnp.float32)).astype(jnp.bfloat16)
    dlow = jnp.dot(dz, up_weight.T, preferred_element_type=jnp.float32).astype(jnp.bfloat16)
    total = batch * lax.axis_size("grp") * owners
    factor = 1.0 / math.sqrt(total)
    part_up = jnp.dot(low.T, dz, preferred_element_type=jnp.float32) * factor
    part_down = jnp.dot(cross_input.T, dlow, preferred_element_type=jnp.float32) * factor
    part_up, part_down = part_up.astype(jnp.bfloat16), part_down.astype(jnp.bfloat16)
    owner_up, owner_down = (
        lax.psum_scatter(part_up, "tbl", scatter_dimension=0, tiled=True).astype(jnp.float32),
        lax.psum_scatter(part_down, "tbl", scatter_dimension=1, tiled=True).astype(jnp.float32),
    )
    got_idx = lax.all_to_all(idx, "tbl", split_axis=0, concat_axis=0, tiled=True)
    pooled = pool(got_idx, tables, batch, maxlen)
    returned = lax.all_to_all(pooled, "tbl", split_axis=0, concat_axis=0, tiled=True)
    next_embedded = order(slot_of_table, returned, width)
    grad_up, grad_down = (
        lax.psum_scatter(owner_up, "grp", scatter_dimension=1, tiled=True),
        lax.psum_scatter(owner_down, "grp", scatter_dimension=0, tiled=True),
    )
    return (next_embedded, grad_up, grad_down)


def step_kernel(
    maxlen,
    factor,
    split,
    checkpoints,
    ids_ref,
    len_ref,
    slot_ref,
    tab_ref,
    x_hbm,
    ct_hbm,
    up_hbm,
    down_hbm,
    emb_ref,
    grad_up_ref,
    grad_down_ref,
    x_ref,
    ct_ref,
    up_ref,
    down_ref,
    idx_ref,
    idx_in,
    idx_s,
    part,
    c_in,
    a_in,
    b_in,
    a2_in,
    b2_in,
    z_in,
    stage,
    wide_even,
    wide_odd,
    acc,
    pooled,
    got,
    tab_sem,
    smem_sem,
    idx_sem,
    core_sem,
    one_sem,
    two_sem,
    z_sem,
    pool_sem,
    load_sem,
):
    owners, zs, _, high, lanes = part.shape
    slots, rows, width = tab_ref.shape
    batch = x_ref.shape[0]
    rank = down_ref.shape[1]
    cols = rank // owners
    chunk = 1024 if rows % 1024 == 0 else 256
    g, t = lax.axis_index("grp"), lax.axis_index("tbl")
    z, x = g // 2, g % 2
    core = t + 1 - 2 * (t % 2)
    far = (t + 2) % owners
    other = 1 - x
    side = g + 1 - 2 * x

    def fetch(s):
        return pltpu.make_async_copy(tab_ref.at[s], stage.at[s % 2], tab_sem.at[s % 2])

    def send(src, dst, sems, n, device):
        return pltpu.make_async_remote_copy(
            src_ref=src,
            dst_ref=dst,
            send_sem=sems.at[0, n],
            recv_sem=sems.at[1, n],
            device_id=device,
            device_id_type=pl.DeviceIdType.MESH,
        )

    loads = [
        pltpu.make_async_copy(a, b, load_sem.at[n])
        for n, (a, b) in enumerate(
            ((x_hbm, x_ref), (down_hbm, down_ref), (ct_hbm, ct_ref), (up_hbm, up_ref))
        )
    ]
    for copy in loads:
        copy.start()
    fetch(0).start()
    barrier = pltpu.get_barrier_semaphore()
    near = [(g, (t + d) % owners) for d in range(1, owners)] + [(side, t)]
    near += [((z + d) % zs * 2 + x, t) for d in range(1, zs)]
    for device in near:
        pl.semaphore_signal(
            barrier, inc=1, device_id=device, device_id_type=pl.DeviceIdType.MESH
        )

    feats, span = slot_ref.shape[0], ids_ref.shape[0]
    each = slots * maxlen
    feat = lax.broadcasted_iota(jnp.int32, (span, feats), 1)
    entry = lax.broadcasted_iota(jnp.int32, (span, feats), 0)
    held_by = jnp.zeros((span, feats), jnp.int32)
    for f in range(feats):
        held_by = jnp.where(feat == f, slot_ref[f], held_by)
    hit = jnp.where(held_by == entry // maxlen, 1.0, 0.0).astype(jnp.bfloat16)
    lens = jnp.dot(
        hit, len_ref[...].astype(jnp.float32).astype(jnp.bfloat16), preferred_element_type=jnp.float32
    )
    place = (lax.broadcasted_iota(jnp.int32, (span, batch), 0) % maxlen).astype(jnp.float32)
    idx = jnp.where(place < lens, ids_ref[...], rows)
    for o in range(owners):
        idx_ref[o] = idx[o * each : (o + 1) * each]

    loads[0].wait()
    loads[1].wait()
    low = jnp.dot(x_ref[...], down_ref[...], preferred_element_type=jnp.float32).astype(jnp.bfloat16)
    loads[2].wait()
    dz = (ct_ref[...].astype(jnp.float32) * x_ref[...].astype(jnp.float32)).astype(jnp.bfloat16)
    loads[3].wait()
    dlow = lax.dot_general(
        dz, up_ref[...], (((1,), (1,)), ((), ())), preferred_element_type=jnp.float32
    ).astype(jnp.bfloat16)
    pl.semaphore_wait(barrier, len(near))

    ids_out = [
        send(idx_ref.at[(t + d) % owners], idx_in.at[t], idx_sem, d - 1, (g, (t + d) % owners))
        for d in range(1, owners)
    ]
    for copy in ids_out:
        copy.start()

    first = (((0,), (0,)), ((), ()))
    for block in range(2 * zs):
        begin = block * high
        edge = begin // LANES * LANES
        stop = -(-(begin + high) // LANES) * LANES
        up = lax.dot_general(dz[:, edge:stop], low, first, preferred_element_type=jnp.float32)
        down = lax.dot_general(
            x_ref[:, edge:stop], dlow, first, preferred_element_type=jnp.float32
        )
        up = (up[begin - edge : begin - edge + high] * factor).astype(jnp.bfloat16)
        down = (down[begin - edge : begin - edge + high] * factor).astype(jnp.bfloat16)
        for o in range(owners):
            part[o, block // 2, block % 2] = jnp.concatenate(
                [up[:, o * cols : (o + 1) * cols], down[:, o * cols : (o + 1) * cols]], axis=1
            )

    cross = [
        send(part.at[core], c_in.at[0], core_sem, 0, (g, core)),
        send(part.at[(core + 2) % owners], c_in.at[1], core_sem, 1, (g, core)),
    ]
    for copy in cross:
        copy.start()

    for copy in ids_out:
        copy.wait()
    idx_in[t] = idx_ref[t]

    def peer(j):
        return (t // 2 + 1 - j // 2) % 2 * 2 + (t + (j + 1) // 2) % 2

    got_ids = [
        [
            pltpu.make_async_copy(
                idx_in.at[peer(j), pl.ds(s * maxlen, maxlen)],
                idx_s.at[s, j],
                smem_sem.at[s * owners + j],
            )
            for j in range(owners)
        ]
        for s in range(slots)
    ]
    for copies in got_ids:
        for copy in copies:
            copy.start()

    low_rows, high_rows = pl.ds(0, split), pl.ds(split, high - split)

    def add(where, value):
        part[where] = (part[where].astype(jnp.float32) + value.astype(jnp.float32)).astype(
            jnp.bfloat16
        )

    one = [
        send(part.at[far, :, :, low_rows], a_in, one_sem, 0, (g, far)),
        send(part.at[t, :, other, high_rows], b_in.at[0], one_sem, 1, (side, t)),
        send(part.at[far, :, other, high_rows], b_in.at[1], one_sem, 2, (side, t)),
    ]
    two = [
        send(part.at[t, :, other, low_rows], a2_in, two_sem, 0, (side, t)),
        send(part.at[far, :, x, high_rows], b2_in, two_sem, 1, (g, far)),
    ]
    last = [
        send(
            part.at[t, (z + d) % zs, x], z_in.at[d - 1], z_sem, d - 1, ((z + d) % zs * 2 + x, t)
        )
        for d in range(1, zs)
    ]

    def after_core():
        for copy in cross:
            copy.wait()
        for n, o in ((1, far), (0, t)):
            for k in range(zs):
                for j in range(2):
                    add((o, k, j), c_in[n, k, j])
        for copy in one:
            copy.start()

    def after_one():
        for copy in one:
            copy.wait()
        for k in range(zs):
            add((t, k, other, low_rows), a_in[k, other])
            add((far, k, x, high_rows), b_in[1, k])
        for copy in two:
            copy.start()
        for k in range(zs):
            add((t, k, x, low_rows), a_in[k, x])
            add((t, k, x, high_rows), b_in[0, k])

    def after_two():
        for copy in two:
            copy.wait()
        for k in range(zs):
            add((t, k, x, low_rows), a2_in[k])
            add((t, k, x, high_rows), b2_in[k])
        for copy in last:
            copy.start()

    stages = [after_core, after_one, after_two]
    wides = (wide_even, wide_odd)

    def widen(s, at):
        wides[s % 2][at, :] = stage[s % 2, at, :].astype(jnp.float32)

    def give(s, j):
        return send(pooled.at[j, s], got.at[t, s], pool_sem, s * (owners - 1) + j, (g, peer(j)))

    for wide in wides:
        wide[pl.ds(rows, 8), :] = jnp.zeros((8, width), jnp.float32)
    fetch(1).start()
    fetch(0).wait()

    @pl.loop(0, rows // chunk)
    def _(c):
        widen(0, pl.ds(pl.multiple_of(c * chunk, chunk), chunk))

    share = rows // owners
    for s in range(slots):
        for copy in got_ids[s]:
            copy.wait()
        if s + 1 < slots:
            fetch(s + 1).wait()
        if s + 2 < slots:
            fetch(s + 2).start()
        wide = wides[s % 2]

        @pl.loop(0, owners)
        def _(j):
            if s + 1 < slots:
                widen(s + 1, pl.ds(pl.multiple_of(j * share, share), share))
            ids = [idx_s.at[s, j, k] for k in range(maxlen)]
            for u in range(batch):
                held = [wide[pl.ds(ids[k][u], 1), :] for k in range(maxlen)]
                while len(held) > 1:
                    held = [a + b for a, b in zip(held[::2], held[1::2])] + (
                        [held[-1]] if len(held) % 2 else []
                    )
                acc[pl.ds(u, 1), :] = held[0]
            pooled[j, s] = acc[...].astype(jnp.bfloat16)

            @pl.when(j < owners - 1)
            def _():
                give(s, j).start()

        for n, at in enumerate(checkpoints):
            if at == s:
                stages[n]()
        got[t, s] = pooled[owners - 1, s]

    for copy in last:
        copy.wait()
    total = part[t, z, x].astype(jnp.float32)
    for d in range(1, zs):
        total += z_in[d - 1].astype(jnp.float32)
    total = total.T
    grad_up_ref[...] = total[:cols]
    grad_down_ref[...] = total[cols:]
    for s in range(slots):
        for j in range(owners - 1):
            give(s, j).wait()
    for f in range(slot_ref.shape[0]):
        s = slot_ref[f]
        emb_ref[:, f * width : (f + 1) * width] = got[lax.div(s, slots), lax.rem(s, slots)]


def fused_step(
    next_ids, next_lengths, slot_of_table, tables, cross_input, cotangent, up_weight, down_weight, maxlen, factor
):
    groups, owners = lax.axis_size("grp"), lax.axis_size("tbl")
    slots, rows, width = tables.shape
    batch, depth = cross_input.shape
    zs, high = groups // 2, depth // groups
    split = (high // 2 + 15) // 16 * 16
    sems = pltpu.SemaphoreType.DMA
    bf16 = jnp.bfloat16
    any_space = pl.BlockSpec(memory_space=pl.ANY)
    idx_shape = (owners, next_ids.shape[1] // owners, batch)
    half = down_weight.shape[1] // owners
    vmem = pl.BlockSpec(memory_space=pltpu.VMEM)
    checkpoints = (0, min(3, slots - 1), min(5, slots - 1))
    return pl.pallas_call(
        functools.partial(step_kernel, maxlen, factor, split, checkpoints),
        out_shape=(
            jax.ShapeDtypeStruct((batch, slot_of_table.shape[0] * width), bf16),
            jax.ShapeDtypeStruct((half, high), jnp.float32),
            jax.ShapeDtypeStruct((half, high), jnp.float32),
        ),
        in_specs=[
            vmem,
            vmem,
            pl.BlockSpec(memory_space=pltpu.SMEM),
            any_space,
            any_space,
            any_space,
            any_space,
            any_space,
        ],
        out_specs=(vmem, vmem, vmem),
        scratch_shapes=[
            pltpu.VMEM(cross_input.shape, bf16),
            pltpu.VMEM(cotangent.shape, bf16),
            pltpu.VMEM(up_weight.shape, bf16),
            pltpu.VMEM(down_weight.shape, bf16),
            pltpu.VMEM(idx_shape, jnp.int32),
            pltpu.VMEM(idx_shape, jnp.int32),
            pltpu.SMEM((slots, owners, maxlen, batch), jnp.int32),
            pltpu.VMEM((owners, zs, 2, high, LANES), bf16),
            pltpu.VMEM((2, zs, 2, high, LANES), bf16),
            pltpu.VMEM((zs, 2, split, LANES), bf16),
            pltpu.VMEM((2, zs, high - split, LANES), bf16),
            pltpu.VMEM((zs, split, LANES), bf16),
            pltpu.VMEM((zs, high - split, LANES), bf16),
            pltpu.VMEM((max(zs - 1, 1), high, LANES), bf16),
            pltpu.VMEM((2, rows, width), bf16),
            pltpu.VMEM((rows + 8, width), jnp.float32),
            pltpu.VMEM((rows + 8, width), jnp.float32),
            pltpu.VMEM((batch, width), jnp.float32),
            pltpu.VMEM((owners, slots, batch, width), bf16),
            pltpu.VMEM((owners, slots, batch, width), bf16),
            sems((2,)),
            sems((slots * owners,)),
            sems((2, owners - 1)),
            sems((2, 2)),
            sems((2, 3)),
            sems((2, 2)),
            sems((2, max(zs - 1, 1))),
            sems((2, slots * (owners - 1))),
            sems((4,)),
        ],
        compiler_params=pltpu.CompilerParams(
            collective_id=0, has_side_effects=True, vmem_limit_bytes=56 << 20
        ),
        name="fused_step",
    )(
        next_ids.T,
        next_lengths.T,
        slot_of_table,
        tables,
        cross_input,
        cotangent,
        up_weight,
        down_weight,
    )


def on_device(
    next_ids, next_lengths, slot_of_table, tables, cross_input, cotangent, up_weight, down_weight
):
    groups, owners = lax.axis_size("grp"), lax.axis_size("tbl")
    batch, depth = cross_input.shape
    rank = down_weight.shape[1]
    slots, rows, _ = tables.shape
    maxlen = next_ids.shape[1] // (slots * owners)
    fits = owners == 4 and groups % 2 == 0 and depth % (16 * groups) == 0 and batch % 16 == 0
    if not fits or rank * 2 != owners * LANES or slots * maxlen % 8 or maxlen != 8 or rows % 1024 or batch != LANES:
        return plain(
            next_ids,
            next_lengths,
            slot_of_table,
            tables,
            cross_input,
            cotangent,
            up_weight,
            down_weight,
        )
    factor = 1.0 / math.sqrt(batch * groups * owners)
    next_embedded, grad_up, grad_down = fused_step(
        next_ids,
        next_lengths,
        slot_of_table,
        tables,
        cross_input,
        cotangent,
        up_weight,
        down_weight,
        maxlen,
        factor,
    )
    return next_embedded, grad_up, grad_down.T


def solution(mesh):
    return jax.shard_map(
        on_device,
        mesh=mesh,
        in_specs=(
            P(("grp", "tbl"), None),
            P(("grp", "tbl"), None),
            P(),
            P("tbl", None, None),
            P(("grp", "tbl"), None),
            P(("grp", "tbl"), None),
            P(),
            P(),
        ),
        out_specs=(P(("grp", "tbl"), None), P("tbl", "grp"), P("grp", "tbl")),
        check_vma=False,
    )
```

```python
import functools
import itertools
import math

import jax
import jax.numpy as jnp
from jax import lax
from jax.experimental import pallas as pl
from jax.experimental.pallas import tpu as pltpu
from jax.sharding import PartitionSpec as P

LANES = 128


def pool_kernel(maxlen, idx_ref, tab_ref, out_ref, stage, wide, acc, sem):
    owners, batch, _ = out_ref.shape
    slots, rows, width = tab_ref.shape
    per_line = LANES // maxlen
    lines = batch // per_line
    chunk = 256

    def fetch(s):
        return pltpu.make_async_copy(tab_ref.at[s], stage.at[s % 2], sem.at[s % 2])

    fetch(0).start()
    wide[pl.ds(rows, 8), :] = jnp.zeros((8, width), jnp.float32)
    for s in range(slots):
        if s + 1 < slots:
            fetch(s + 1).start()
        fetch(s).wait()

        @pl.loop(0, rows // chunk)
        def _(c):
            at = pl.ds(pl.multiple_of(c * chunk, chunk), chunk)
            wide[at, :] = stage[s % 2, at, :].astype(jnp.float32)

        @pl.loop(0, owners * lines)
        def _(g):
            src = g // lines
            line = s * lines + g % lines
            for u in range(per_line):
                got = [
                    wide[pl.ds(idx_ref[src, line, u * maxlen + k], 1), :] for k in range(maxlen)
                ]
                while len(got) > 1:
                    got = [a + b for a, b in zip(got[::2], got[1::2])] + (
                        [got[-1]] if len(got) % 2 else []
                    )
                acc[pl.ds(g * per_line + u, 1), :] = got[0]

        for o in range(owners):
            out_ref[o, :, s * width : (s + 1) * width] = acc[
                o * batch : (o + 1) * batch, :
            ].astype(jnp.bfloat16)


def pool(idx, tables, batch, maxlen):
    slots, rows, width = tables.shape
    owners = idx.shape[0]
    return pl.pallas_call(
        functools.partial(pool_kernel, maxlen),
        out_shape=jax.ShapeDtypeStruct((owners, batch, slots * width), jnp.bfloat16),
        in_specs=[
            pl.BlockSpec(memory_space=pltpu.SMEM),
            pl.BlockSpec(memory_space=pl.ANY),
        ],
        out_specs=pl.BlockSpec(memory_space=pltpu.VMEM),
        scratch_shapes=[
            pltpu.VMEM((2, rows, width), jnp.bfloat16),
            pltpu.VMEM((rows + 8, width), jnp.float32),
            pltpu.VMEM((owners * batch, width), jnp.float32),
            pltpu.SemaphoreType.DMA((2,)),
        ],
        compiler_params=pltpu.CompilerParams(vmem_limit_bytes=60 << 20),
        cost_estimate=pl.CostEstimate(
            flops=100_000_000, bytes_accessed=tables.size * 2, transcendentals=0
        ),
        name="pool",
    )(idx, tables)


def order_kernel(slot_ref, got_ref, out_ref):
    owners, batch, wide = got_ref.shape
    feats = slot_ref.shape[0]
    width = out_ref.shape[1] // feats
    slots = wide // width
    for f in range(feats):
        s = slot_ref[f]
        at = pl.ds(pl.multiple_of(lax.rem(s, slots) * width, width), width)
        out_ref[:, f * width : (f + 1) * width] = got_ref[lax.div(s, slots), :, at]


def order(slot_of_table, got, width):
    return pl.pallas_call(
        order_kernel,
        out_shape=jax.ShapeDtypeStruct(
            (got.shape[1], slot_of_table.shape[0] * width), jnp.bfloat16
        ),
        in_specs=[
            pl.BlockSpec(memory_space=pltpu.SMEM),
            pl.BlockSpec(memory_space=pltpu.VMEM),
        ],
        out_specs=pl.BlockSpec(memory_space=pltpu.VMEM),
        name="order",
    )(slot_of_table, got)


def bag_rows(next_ids, next_lengths, slot_of_table, slots, owners, rows):
    batch = next_ids.shape[0]
    slots_all = slots * owners
    maxlen = next_ids.shape[1] // slots_all
    hit = (slot_of_table[:, None] == lax.broadcasted_iota(jnp.int32, (1, slots_all), 1)).astype(
        jnp.int32
    )
    slot_lengths = jnp.sum(next_lengths[:, :, None] * hit[None, :, :], axis=1)
    keep = lax.broadcasted_iota(jnp.int32, (batch, slots_all, maxlen), 2) < slot_lengths[:, :, None]
    idx = jnp.where(keep, next_ids.reshape(batch, slots_all, maxlen), rows)
    return idx.transpose(1, 0, 2).reshape(owners, slots * batch * maxlen // LANES, LANES)


def plain(
    next_ids, next_lengths, slot_of_table, tables, cross_input, cotangent, up_weight, down_weight
):
    batch = next_ids.shape[0]
    owners = lax.axis_size("tbl")
    slots, rows, width = tables.shape
    maxlen = next_ids.shape[1] // (slots * owners)
    idx = bag_rows(next_ids, next_lengths, slot_of_table, slots, owners, rows)
    low = jnp.dot(cross_input, down_weight, preferred_element_type=jnp.float32).astype(jnp.bfloat16)
    dz = (cotangent.astype(jnp.float32) * cross_input.astype(jnp.float32)).astype(jnp.bfloat16)
    dlow = jnp.dot(dz, up_weight.T, preferred_element_type=jnp.float32).astype(jnp.bfloat16)
    total = batch * lax.axis_size("grp") * owners
    factor = 1.0 / math.sqrt(total)
    part_up = jnp.dot(low.T, dz, preferred_element_type=jnp.float32) * factor
    part_down = jnp.dot(cross_input.T, dlow, preferred_element_type=jnp.float32) * factor
    part_up, part_down = part_up.astype(jnp.bfloat16), part_down.astype(jnp.bfloat16)
    owner_up, owner_down = (
        lax.psum_scatter(part_up, "tbl", scatter_dimension=0, tiled=True).astype(jnp.float32),
        lax.psum_scatter(part_down, "tbl", scatter_dimension=1, tiled=True).astype(jnp.float32),
    )
    got_idx = lax.all_to_all(idx, "tbl", split_axis=0, concat_axis=0, tiled=True)
    pooled = pool(got_idx, tables, batch, maxlen)
    returned = lax.all_to_all(pooled, "tbl", split_axis=0, concat_axis=0, tiled=True)
    next_embedded = order(slot_of_table, returned, width)
    grad_up, grad_down = (
        lax.psum_scatter(owner_up, "grp", scatter_dimension=1, tiled=True),
        lax.psum_scatter(owner_down, "grp", scatter_dimension=0, tiled=True),
    )
    return (next_embedded, grad_up, grad_down)


PLAN = (("uxyv", 5), ("yuxv", 3), ("xyuv", 2), ("xuvy", 4))
POLLS = ((12, 3, 0), (13, 0, 0), (15, 2, 0), (15, 1, 0), (21, 3, 1), (22, 2, 1), (23, 1, 1), (23, 0, 1), (28, 1, 2), (28, 2, 2), (28, 0, 2), (28, 3, 2), (28, 2, 3), (28, 3, 3), (28, 1, 3), (28, 0, 3))
LATE = ((2, 7),)


def step_kernel(
    maxlen,
    ids_hbm,
    len_hbm,
    slot_hbm,
    tab_ref,
    x_hbm,
    ct_hbm,
    up_hbm,
    down_hbm,
    got,
    out_ref,
    ids_ref,
    len_ref,
    slot_ref,
    x_ref,
    ct_ref,
    up_ref,
    down_ref,
    xt,
    dzt,
    x_in,
    dz_in,
    low_ref,
    dlow_ref,
    low_in,
    dlow_in,
    idx_ref,
    idx_in,
    idx_s,
    part,
    fin,
    fin_out,
    fin_in,
    full,
    stage,
    wide_even,
    wide_odd,
    acc,
    pooled,
    tab_sem,
    smem_sem,
    idx_sem,
    mate_sem,
    class_sem,
    fin_sem,
    pool_sem,
    load_sem,
    *landing,
):
    slots, rows, width = tab_ref.shape
    batch, depth = x_ref.shape
    rank = down_ref.shape[1]
    half = x_in.shape[1]
    owners, groups = 4, 8
    high = depth // groups
    cols = rank // owners
    chunk = 1024
    g, t = lax.axis_index("grp"), lax.axis_index("tbl")
    core = t % 2
    at_axis = {"y": t // 2, "v": g // 4, "u": g // 2 % 2, "x": g % 2}
    mate = (g, t + 1 - 2 * core)
    across = {
        "y": (g, (t + 2) % owners),
        "v": ((g + 4) % groups, t),
        "u": (g + 2 - 4 * at_axis["u"], t),
        "x": (g + 1 - 2 * at_axis["x"], t),
    }

    def fetch(s):
        return pltpu.make_async_copy(tab_ref.at[s], stage.at[s % 2], tab_sem.at[s % 2])

    def send(src, dst, sems, n, device):
        return pltpu.make_async_remote_copy(
            src_ref=src,
            dst_ref=dst,
            send_sem=sems.at[0, n],
            recv_sem=sems.at[1, n],
            device_id=device,
            device_id_type=pl.DeviceIdType.MESH,
        )

    loads = [
        pltpu.make_async_copy(a, b, load_sem.at[n])
        for n, (a, b) in enumerate(
            (
                (ids_hbm, ids_ref),
                (len_hbm, len_ref),
                (slot_hbm, slot_ref),
                (x_hbm, x_ref),
                (down_hbm, down_ref),
                (ct_hbm, ct_ref),
                (up_hbm, up_ref),
            )
        )
    ]
    for copy in loads:
        copy.start()
    fetch(0).start()
    barrier = pltpu.get_barrier_semaphore()
    near = [(g, (t + d) % owners) for d in range(1, owners)] + [across[d] for d in "vux"]
    for device in near:
        pl.semaphore_signal(
            barrier, inc=1, device_id=device, device_id_type=pl.DeviceIdType.MESH
        )

    for copy in loads[:3]:
        copy.wait()
    feats, span = slot_ref.shape[1], ids_ref.shape[0]
    each = slots * maxlen
    entry = lax.broadcasted_iota(jnp.int32, (span, feats), 0)
    hit = jnp.where(slot_ref[...] == entry // maxlen, 1.0, 0.0).astype(jnp.bfloat16)
    lens = jnp.dot(
        hit, len_ref[...].astype(jnp.float32).astype(jnp.bfloat16), preferred_element_type=jnp.float32
    )
    place = (lax.broadcasted_iota(jnp.int32, (span, batch), 0) % maxlen).astype(jnp.float32)
    idx = jnp.where(place < lens, ids_ref[...], rows)
    for o in range(owners):
        idx_ref[o] = idx[o * each : (o + 1) * each]

    def turn(src, dst):
        for n in range(depth // LANES):
            at = slice(n * LANES, (n + 1) * LANES)
            dst[at, :] = src[:, at].T

    loads[3].wait()
    turn(x_ref, xt)
    loads[4].wait()
    low_ref[...] = jnp.dot(
        x_ref[...], down_ref[...], preferred_element_type=jnp.float32
    ).astype(jnp.bfloat16)

    pl.semaphore_wait(barrier, len(near))

    ids_out = [
        send(idx_ref.at[(t + d) % owners], idx_in.at[t], idx_sem, d - 1, (g, (t + d) % owners))
        for d in range(1, owners)
    ]

    def lend(src, dst, n):
        return [
            send(
                src.at[pl.ds(pl.multiple_of(b * high + (1 - core) * (high - half), 16), half)],
                dst.at[b],
                mate_sem,
                n + b,
                mate,
            )
            for b in range(groups)
        ]

    x_out, dz_out = lend(xt, x_in, 0), lend(dzt, dz_in, groups)
    low_out = send(low_ref, low_in, mate_sem, 2 * groups, mate)
    dlow_out = send(dlow_ref, dlow_in, mate_sem, 2 * groups + 1, mate)
    for copy in ids_out + x_out + [low_out]:
        copy.start()

    loads[5].wait()
    ct_ref[...] = (ct_ref[...].astype(jnp.float32) * x_ref[...].astype(jnp.float32)).astype(
        jnp.bfloat16
    )
    turn(ct_ref, dzt)
    for copy in dz_out:
        copy.start()
    loads[6].wait()
    dlow = lax.dot_general(
        ct_ref[...], up_ref[...], (((1,), (1,)), ((), ())), preferred_element_type=jnp.float32
    ).astype(jnp.bfloat16)
    swap = [n + 1 - 2 * (n % 2) for n in range(owners)]
    dlow_ref[...] = jnp.concatenate([dlow[:, n * cols : (n + 1) * cols] for n in swap], axis=1)
    dlow_out.start()

    wides = (wide_even, wide_odd)

    def widen(s, at):
        wides[s % 2][at, :] = stage[s % 2, at, :].astype(jnp.float32)

    for wide in wides:
        wide[pl.ds(rows, 8), :] = jnp.zeros((8, width), jnp.float32)
    fetch(1).start()
    fetch(0).wait()

    @pl.loop(0, rows // chunk)
    def _(c):
        widen(0, pl.ds(pl.multiple_of(c * chunk, chunk), chunk))

    for copy in ids_out:
        copy.wait()
    idx_in[t] = idx_ref[t]

    def peer(j):
        return (t // 2 + 1 - j // 2) % 2 * 2 + (t + (j + 1) // 2) % 2

    got_ids = [
        [
            pltpu.make_async_copy(
                idx_in.at[peer(j), pl.ds(s * maxlen, maxlen)],
                idx_s.at[s, j],
                smem_sem.at[s * owners + j],
            )
            for j in range(owners)
        ]
        for s in range(slots)
    ]
    for copies in got_ids:
        for copy in copies:
            copy.start()

    for copy in x_out + dz_out + [low_out, dlow_out]:
        copy.wait()
    low_two = jnp.concatenate([low_ref[...], low_in[...]], axis=0)
    dlow_two = jnp.concatenate([dlow_ref[...], dlow_in[...]], axis=0)
    left = lax.broadcasted_iota(jnp.int32, (half, LANES), 1) < cols
    for b in range(groups):
        at = pl.ds(pl.multiple_of(b * high + core * (high - half), 16), half)
        up = jnp.dot(
            jnp.concatenate([dzt[at, :], dz_in[b]], axis=1),
            low_two,
            preferred_element_type=jnp.float32,
        )
        down = jnp.dot(
            jnp.concatenate([xt[at, :], x_in[b]], axis=1),
            dlow_two,
            preferred_element_type=jnp.float32,
        )
        for y in range(2):
            u, d = up[:, y * LANES : (y + 1) * LANES], down[:, y * LANES : (y + 1) * LANES]
            part[y, 0, b // 4, b // 2 % 2, b % 2] = jnp.where(left, u, d).astype(jnp.bfloat16)
            part[y, 1, b // 4, b // 2 % 2, b % 2] = jnp.where(left, d, u).astype(jnp.bfloat16)

    begins = [sum(n for _, n in PLAN[:k]) * half // 14 for k in range(len(PLAN) + 1)]

    def place_of(k, held):
        span = pl.ds(begins[k], begins[k + 1] - begins[k])
        return tuple(held.get(d, slice(None)) for d in "ycvux") + (span,)

    def exchange(k, i):
        order = PLAN[k][0]
        held = {d: at_axis[d] for d in order[:i]}
        held[order[i]] = 1 - at_axis[order[i]]
        return send(
            part.at[place_of(k, held)], landing[4 * k + i], class_sem, 4 * k + i, across[order[i]]
        )

    def hand(k):
        span = pl.ds(begins[k], begins[k + 1] - begins[k])
        return send(fin_out.at[span], fin_in.at[span], fin_sem, k, mate)

    def take(k, i):
        exchange(k, i).wait()
        order, came = PLAN[k][0], landing[4 * k + i]
        held = {d: at_axis[d] for d in order[: i + 1]}
        span = pl.ds(begins[k], begins[k + 1] - begins[k])
        if i == 3:
            for c, keep in ((1 - core, False), (core, True)):
                total = part[place_of(k, held | {"c": c})].astype(jnp.float32) + came[c].astype(
                    jnp.float32
                )
                if keep:
                    fin[span, :] = total
                else:
                    fin_out[span, :] = total.astype(jnp.bfloat16)
                    hand(k).start()
            return
        free = [d for d in "ycvux" if d not in held]
        for pick in itertools.product(range(2), repeat=len(free)):
            at = place_of(k, held | dict(zip(free, pick)))
            part[at] = (part[at].astype(jnp.float32) + came[pick].astype(jnp.float32)).astype(
                jnp.bfloat16
            )
        exchange(k, i + 1).start()

    for k in range(len(PLAN)):
        if k not in dict(LATE):
            exchange(k, 0).start()

    def give(s, j):
        return send(pooled.at[j, s], got.at[t, s], pool_sem, s * (owners - 1) + j, (g, peer(j)))

    share = rows // owners
    for s in range(slots):
        for copy in got_ids[s]:
            copy.wait()
        if s + 1 < slots:
            fetch(s + 1).wait()
        if s + 2 < slots:
            fetch(s + 2).start()
        wide = wides[s % 2]

        @pl.loop(0, owners)
        def _(j):
            if s + 1 < slots:
                widen(s + 1, pl.ds(pl.multiple_of(j * share, share), share))
            ids = [idx_s.at[s, j, k] for k in range(maxlen)]
            for u in range(batch):
                held = [wide[pl.ds(ids[k][u], 1), :] for k in range(maxlen)]
                while len(held) > 1:
                    held = [a + b for a, b in zip(held[::2], held[1::2])]
                acc[pl.ds(u, 1), :] = held[0]
            pooled[j, s] = acc[...].astype(jnp.bfloat16)

            @pl.when(j < owners - 1)
            def _():
                give(s, j).start()

            for n in range(owners):
                now = s * owners + n
                todo = [p for p in POLLS if p[0] == now]
                begin = [k for k, p in LATE if p == now]
                if todo or begin:

                    @pl.when(j == n)
                    def _():
                        for _, k, i in todo:
                            take(k, i)
                        for k in begin:
                            exchange(k, 0).start()

        got[t, s] = pooled[owners - 1, s]

    for now, k, i in POLLS:
        if now >= slots * owners:
            take(k, i)
    for k in range(len(PLAN)):
        hand(k).wait()
    other = pl.ds(pl.multiple_of((1 - core) * (high - half), 16), half)
    own = pl.ds(pl.multiple_of(core * (high - half), 16), half)
    full[other, :] = fin_in[...].astype(jnp.float32)
    full[own, :] = fin[...]
    total = full[...].T
    out_ref[core] = total[:cols]
    out_ref[1 - core] = total[cols:]
    for s in range(slots):
        for j in range(owners - 1):
            give(s, j).wait()


def fused_step(
    next_ids, next_lengths, slot_of_table, tables, cross_input, cotangent, up_weight, down_weight, maxlen
):
    groups, owners = lax.axis_size("grp"), lax.axis_size("tbl")
    slots, rows, width = tables.shape
    batch, depth = cross_input.shape
    rank = down_weight.shape[1]
    high = depth // groups
    half = (high // 2 + 15) // 16 * 16
    sems = pltpu.SemaphoreType.DMA
    bf16, f32 = jnp.bfloat16, jnp.float32
    any_space = pl.BlockSpec(memory_space=pl.ANY)
    idx_shape = (owners, next_ids.shape[1] // owners, batch)
    vmem = pl.BlockSpec(memory_space=pltpu.VMEM)
    landing = [
        pltpu.VMEM((2,) * (4 - i) + (n * half // 14, LANES), bf16)
        for _, n in PLAN
        for i in range(4)
    ]
    return pl.pallas_call(
        functools.partial(step_kernel, maxlen),
        out_shape=(
            jax.ShapeDtypeStruct((owners, slots, batch, width), bf16),
            jax.ShapeDtypeStruct((2, rank // owners, high), f32),
        ),
        in_specs=[any_space] * 8,
        out_specs=(vmem, vmem),
        scratch_shapes=[
            pltpu.VMEM(next_ids.shape[::-1], jnp.int32),
            pltpu.VMEM(next_lengths.shape[::-1], jnp.int32),
            pltpu.VMEM((1, slot_of_table.shape[0]), jnp.int32),
            pltpu.VMEM(cross_input.shape, bf16),
            pltpu.VMEM(cotangent.shape, bf16),
            pltpu.VMEM(up_weight.shape, bf16),
            pltpu.VMEM(down_weight.shape, bf16),
            pltpu.VMEM((depth, batch), bf16),
            pltpu.VMEM((depth, batch), bf16),
            pltpu.VMEM((groups, half, batch), bf16),
            pltpu.VMEM((groups, half, batch), bf16),
            pltpu.VMEM((batch, rank), bf16),
            pltpu.VMEM((batch, rank), bf16),
            pltpu.VMEM((batch, rank), bf16),
            pltpu.VMEM((batch, rank), bf16),
            pltpu.VMEM(idx_shape, jnp.int32),
            pltpu.VMEM(idx_shape, jnp.int32),
            pltpu.SMEM((slots, owners, maxlen, batch), jnp.int32),
            pltpu.VMEM((2, 2, 2, 2, 2, half, LANES), bf16),
            pltpu.VMEM((half, LANES), f32),
            pltpu.VMEM((half, LANES), bf16),
            pltpu.VMEM((half, LANES), bf16),
            pltpu.VMEM((high, LANES), f32),
            pltpu.VMEM((2, rows, width), bf16),
            pltpu.VMEM((rows + 8, width), f32),
            pltpu.VMEM((rows + 8, width), f32),
            pltpu.VMEM((batch, width), f32),
            pltpu.VMEM((owners, slots, batch, width), bf16),
            sems((2,)),
            sems((slots * owners,)),
            sems((2, owners - 1)),
            sems((2, 2 * groups + 2)),
            sems((2, 4 * len(PLAN))),
            sems((2, len(PLAN))),
            sems((2, slots * (owners - 1))),
            sems((7,)),
        ]
        + landing,
        compiler_params=pltpu.CompilerParams(
            collective_id=0, has_side_effects=True, vmem_limit_bytes=48 << 20
        ),
        name="fused_step",
    )(
        next_ids.T,
        next_lengths.T,
        slot_of_table[None, :],
        tables,
        cross_input,
        cotangent,
        up_weight,
        down_weight,
    )


def finish_kernel(factor, slot_ref, got_ref, sum_ref, emb_ref, grad_up_ref, grad_down_ref):
    slots, _, width = got_ref.shape[1:]
    for f in range(slot_ref.shape[0]):
        s = slot_ref[f]
        emb_ref[:, f * width : (f + 1) * width] = got_ref[lax.div(s, slots), lax.rem(s, slots)]
    grad_up_ref[...] = sum_ref[0] * factor
    grad_down_ref[...] = sum_ref[1] * factor


def finish(slot_of_table, got, sums, factor):
    _, _, batch, width = got.shape
    vmem = pl.BlockSpec(memory_space=pltpu.VMEM)
    return pl.pallas_call(
        functools.partial(finish_kernel, factor),
        out_shape=(
            jax.ShapeDtypeStruct((batch, slot_of_table.shape[0] * width), jnp.bfloat16),
            jax.ShapeDtypeStruct(sums.shape[1:], jnp.float32),
            jax.ShapeDtypeStruct(sums.shape[1:], jnp.float32),
        ),
        in_specs=[pl.BlockSpec(memory_space=pltpu.SMEM), vmem, vmem],
        out_specs=(vmem, vmem, vmem),
        name="finish",
    )(slot_of_table, got, sums)


def on_device(
    next_ids, next_lengths, slot_of_table, tables, cross_input, cotangent, up_weight, down_weight
):
    groups, owners = lax.axis_size("grp"), lax.axis_size("tbl")
    batch, depth = cross_input.shape
    rank = down_weight.shape[1]
    slots, rows, _ = tables.shape
    maxlen = next_ids.shape[1] // (slots * owners)
    fits = (
        owners == 4
        and groups == 8
        and depth % (16 * groups) == 0
        and depth % LANES == 0
        and depth // groups <= 448
        and depth // groups > 432 - 16
        and rank == 256
        and maxlen == 8
        and slots > 2
        and rows % 1024 == 0
        and batch == LANES
    )
    args = (
        next_ids,
        next_lengths,
        slot_of_table,
        tables,
        cross_input,
        cotangent,
        up_weight,
        down_weight,
    )
    if not fits:
        return plain(*args)
    got, sums = fused_step(*args, maxlen)
    factor = 1.0 / math.sqrt(batch * groups * owners)
    next_embedded, grad_up, grad_down = finish(slot_of_table, got, sums, factor)
    return next_embedded, grad_up, grad_down.T


def solution(mesh):
    return jax.shard_map(
        on_device,
        mesh=mesh,
        in_specs=(
            P(("grp", "tbl"), None),
            P(("grp", "tbl"), None),
            P(),
            P("tbl", None, None),
            P(("grp", "tbl"), None),
            P(("grp", "tbl"), None),
            P(),
            P(),
        ),
        out_specs=(P(("grp", "tbl"), None), P("tbl", "grp"), P("grp", "tbl")),
        check_vma=False,
    )
```

```python
import functools
import itertools
import math

import jax
import jax.numpy as jnp
from jax import lax
from jax.experimental import pallas as pl
from jax.experimental.pallas import tpu as pltpu
from jax.sharding import PartitionSpec as P

LANES = 128


def pool_kernel(maxlen, idx_ref, tab_ref, out_ref, stage, wide, acc, sem):
    owners, batch, _ = out_ref.shape
    slots, rows, width = tab_ref.shape
    per_line = LANES // maxlen
    lines = batch // per_line
    chunk = 256

    def fetch(s):
        return pltpu.make_async_copy(tab_ref.at[s], stage.at[s % 2], sem.at[s % 2])

    fetch(0).start()
    wide[pl.ds(rows, 8), :] = jnp.zeros((8, width), jnp.float32)
    for s in range(slots):
        if s + 1 < slots:
            fetch(s + 1).start()
        fetch(s).wait()

        @pl.loop(0, rows // chunk)
        def _(c):
            at = pl.ds(pl.multiple_of(c * chunk, chunk), chunk)
            wide[at, :] = stage[s % 2, at, :].astype(jnp.float32)

        @pl.loop(0, owners * lines)
        def _(g):
            src = g // lines
            line = s * lines + g % lines
            for u in range(per_line):
                got = [
                    wide[pl.ds(idx_ref[src, line, u * maxlen + k], 1), :] for k in range(maxlen)
                ]
                while len(got) > 1:
                    got = [a + b for a, b in zip(got[::2], got[1::2])] + (
                        [got[-1]] if len(got) % 2 else []
                    )
                acc[pl.ds(g * per_line + u, 1), :] = got[0]

        for o in range(owners):
            out_ref[o, :, s * width : (s + 1) * width] = acc[
                o * batch : (o + 1) * batch, :
            ].astype(jnp.bfloat16)


def pool(idx, tables, batch, maxlen):
    slots, rows, width = tables.shape
    owners = idx.shape[0]
    return pl.pallas_call(
        functools.partial(pool_kernel, maxlen),
        out_shape=jax.ShapeDtypeStruct((owners, batch, slots * width), jnp.bfloat16),
        in_specs=[
            pl.BlockSpec(memory_space=pltpu.SMEM),
            pl.BlockSpec(memory_space=pl.ANY),
        ],
        out_specs=pl.BlockSpec(memory_space=pltpu.VMEM),
        scratch_shapes=[
            pltpu.VMEM((2, rows, width), jnp.bfloat16),
            pltpu.VMEM((rows + 8, width), jnp.float32),
            pltpu.VMEM((owners * batch, width), jnp.float32),
            pltpu.SemaphoreType.DMA((2,)),
        ],
        compiler_params=pltpu.CompilerParams(vmem_limit_bytes=60 << 20),
        cost_estimate=pl.CostEstimate(
            flops=100_000_000, bytes_accessed=tables.size * 2, transcendentals=0
        ),
        name="pool",
    )(idx, tables)


def order_kernel(slot_ref, got_ref, out_ref):
    owners, batch, wide = got_ref.shape
    feats = slot_ref.shape[0]
    width = out_ref.shape[1] // feats
    slots = wide // width
    for f in range(feats):
        s = slot_ref[f]
        at = pl.ds(pl.multiple_of(lax.rem(s, slots) * width, width), width)
        out_ref[:, f * width : (f + 1) * width] = got_ref[lax.div(s, slots), :, at]


def order(slot_of_table, got, width):
    return pl.pallas_call(
        order_kernel,
        out_shape=jax.ShapeDtypeStruct(
            (got.shape[1], slot_of_table.shape[0] * width), jnp.bfloat16
        ),
        in_specs=[
            pl.BlockSpec(memory_space=pltpu.SMEM),
            pl.BlockSpec(memory_space=pltpu.VMEM),
        ],
        out_specs=pl.BlockSpec(memory_space=pltpu.VMEM),
        name="order",
    )(slot_of_table, got)


def bag_rows(next_ids, next_lengths, slot_of_table, slots, owners, rows):
    batch = next_ids.shape[0]
    slots_all = slots * owners
    maxlen = next_ids.shape[1] // slots_all
    hit = (slot_of_table[:, None] == lax.broadcasted_iota(jnp.int32, (1, slots_all), 1)).astype(
        jnp.int32
    )
    slot_lengths = jnp.sum(next_lengths[:, :, None] * hit[None, :, :], axis=1)
    keep = lax.broadcasted_iota(jnp.int32, (batch, slots_all, maxlen), 2) < slot_lengths[:, :, None]
    idx = jnp.where(keep, next_ids.reshape(batch, slots_all, maxlen), rows)
    return idx.transpose(1, 0, 2).reshape(owners, slots * batch * maxlen // LANES, LANES)


def plain(
    next_ids, next_lengths, slot_of_table, tables, cross_input, cotangent, up_weight, down_weight
):
    batch = next_ids.shape[0]
    owners = lax.axis_size("tbl")
    slots, rows, width = tables.shape
    maxlen = next_ids.shape[1] // (slots * owners)
    idx = bag_rows(next_ids, next_lengths, slot_of_table, slots, owners, rows)
    low = jnp.dot(cross_input, down_weight, preferred_element_type=jnp.float32).astype(jnp.bfloat16)
    dz = (cotangent.astype(jnp.float32) * cross_input.astype(jnp.float32)).astype(jnp.bfloat16)
    dlow = jnp.dot(dz, up_weight.T, preferred_element_type=jnp.float32).astype(jnp.bfloat16)
    total = batch * lax.axis_size("grp") * owners
    factor = 1.0 / math.sqrt(total)
    part_up = jnp.dot(low.T, dz, preferred_element_type=jnp.float32) * factor
    part_down = jnp.dot(cross_input.T, dlow, preferred_element_type=jnp.float32) * factor
    part_up, part_down = part_up.astype(jnp.bfloat16), part_down.astype(jnp.bfloat16)
    owner_up, owner_down = (
        lax.psum_scatter(part_up, "tbl", scatter_dimension=0, tiled=True).astype(jnp.float32),
        lax.psum_scatter(part_down, "tbl", scatter_dimension=1, tiled=True).astype(jnp.float32),
    )
    got_idx = lax.all_to_all(idx, "tbl", split_axis=0, concat_axis=0, tiled=True)
    pooled = pool(got_idx, tables, batch, maxlen)
    returned = lax.all_to_all(pooled, "tbl", split_axis=0, concat_axis=0, tiled=True)
    next_embedded = order(slot_of_table, returned, width)
    grad_up, grad_down = (
        lax.psum_scatter(owner_up, "grp", scatter_dimension=1, tiled=True),
        lax.psum_scatter(owner_down, "grp", scatter_dimension=0, tiled=True),
    )
    return (next_embedded, grad_up, grad_down)


PLAN = (("uxyv", 5), ("yuxv", 3), ("xyuv", 2), ("xuvy", 4))
POLLS = ((12, 3, 0), (13, 0, 0), (15, 2, 0), (15, 1, 0), (21, 3, 1), (22, 2, 1), (23, 1, 1), (23, 0, 1), (28, 1, 2), (28, 2, 2), (28, 0, 2), (28, 3, 2), (28, 2, 3), (28, 3, 3), (28, 1, 3), (28, 0, 3))
LATE = ((2, 7),)


def step_kernel(
    maxlen,
    factor,
    ids_hbm,
    len_hbm,
    slot_hbm,
    tab_ref,
    x_hbm,
    ct_hbm,
    up_hbm,
    down_hbm,
    got,
    out_ref,
    ids_ref,
    len_ref,
    slot_ref,
    x_ref,
    ct_ref,
    up_ref,
    down_ref,
    xt,
    dzt,
    x_in,
    dz_in,
    low_ref,
    dlow_ref,
    low_in,
    dlow_in,
    idx_ref,
    idx_in,
    idx_s,
    part,
    fin,
    fin_out,
    fin_in,
    full,
    stage,
    wide_even,
    wide_odd,
    acc,
    pooled,
    tab_sem,
    smem_sem,
    idx_sem,
    mate_sem,
    class_sem,
    fin_sem,
    pool_sem,
    load_sem,
    *landing,
):
    slots, rows, width = tab_ref.shape
    batch, depth = x_ref.shape
    rank = down_ref.shape[1]
    half = x_in.shape[1]
    owners, groups = 4, 8
    high = depth // groups
    cols = rank // owners
    chunk = 1024
    g, t = lax.axis_index("grp"), lax.axis_index("tbl")
    core = t % 2
    at_axis = {"y": t // 2, "v": g // 4, "u": g // 2 % 2, "x": g % 2}
    mate = (g, t + 1 - 2 * core)
    across = {
        "y": (g, (t + 2) % owners),
        "v": ((g + 4) % groups, t),
        "u": (g + 2 - 4 * at_axis["u"], t),
        "x": (g + 1 - 2 * at_axis["x"], t),
    }

    def fetch(s):
        return pltpu.make_async_copy(tab_ref.at[s], stage.at[s % 2], tab_sem.at[s % 2])

    def send(src, dst, sems, n, device):
        return pltpu.make_async_remote_copy(
            src_ref=src,
            dst_ref=dst,
            send_sem=sems.at[0, n],
            recv_sem=sems.at[1, n],
            device_id=device,
            device_id_type=pl.DeviceIdType.MESH,
        )

    loads = [
        pltpu.make_async_copy(a, b, load_sem.at[n])
        for n, (a, b) in enumerate(
            (
                (ids_hbm, ids_ref),
                (len_hbm, len_ref),
                (slot_hbm, slot_ref),
                (x_hbm, x_ref),
                (down_hbm, down_ref),
                (ct_hbm, ct_ref),
                (up_hbm, up_ref),
            )
        )
    ]
    for copy in loads:
        copy.start()
    fetch(0).start()
    barrier = pltpu.get_barrier_semaphore()
    near = [(g, (t + d) % owners) for d in range(1, owners)] + [across[d] for d in "vux"]
    for device in near:
        pl.semaphore_signal(
            barrier, inc=1, device_id=device, device_id_type=pl.DeviceIdType.MESH
        )

    for copy in loads[:3]:
        copy.wait()
    feats, span = slot_ref.shape[1], ids_ref.shape[0]
    each = slots * maxlen
    entry = lax.broadcasted_iota(jnp.int32, (span, feats), 0)
    hit = jnp.where(slot_ref[...] == entry // maxlen, 1.0, 0.0).astype(jnp.bfloat16)
    lens = jnp.dot(
        hit, len_ref[...].astype(jnp.float32).astype(jnp.bfloat16), preferred_element_type=jnp.float32
    )
    place = (lax.broadcasted_iota(jnp.int32, (span, batch), 0) % maxlen).astype(jnp.float32)
    idx = jnp.where(place < lens, ids_ref[...], rows)
    for o in range(owners):
        idx_ref[o] = idx[o * each : (o + 1) * each]

    def turn(src, dst):
        for n in range(depth // LANES):
            at = slice(n * LANES, (n + 1) * LANES)
            dst[at, :] = src[:, at].T

    loads[3].wait()
    turn(x_ref, xt)
    loads[4].wait()
    low_ref[...] = jnp.dot(
        x_ref[...], down_ref[...], preferred_element_type=jnp.float32
    ).astype(jnp.bfloat16)

    pl.semaphore_wait(barrier, len(near))

    ids_out = [
        send(idx_ref.at[(t + d) % owners], idx_in.at[t], idx_sem, d - 1, (g, (t + d) % owners))
        for d in range(1, owners)
    ]

    def lend(src, dst, n):
        return [
            send(
                src.at[pl.ds(pl.multiple_of(b * high + (1 - core) * (high - half), 16), half)],
                dst.at[b],
                mate_sem,
                n + b,
                mate,
            )
            for b in range(groups)
        ]

    x_out, dz_out = lend(xt, x_in, 0), lend(dzt, dz_in, groups)
    low_out = send(low_ref, low_in, mate_sem, 2 * groups, mate)
    dlow_out = send(dlow_ref, dlow_in, mate_sem, 2 * groups + 1, mate)
    for copy in ids_out + x_out + [low_out]:
        copy.start()

    loads[5].wait()
    ct_ref[...] = (ct_ref[...].astype(jnp.float32) * x_ref[...].astype(jnp.float32)).astype(
        jnp.bfloat16
    )
    turn(ct_ref, dzt)
    for copy in dz_out:
        copy.start()
    loads[6].wait()
    dlow = lax.dot_general(
        ct_ref[...], up_ref[...], (((1,), (1,)), ((), ())), preferred_element_type=jnp.float32
    ).astype(jnp.bfloat16)
    swap = [n + 1 - 2 * (n % 2) for n in range(owners)]
    dlow_ref[...] = jnp.concatenate([dlow[:, n * cols : (n + 1) * cols] for n in swap], axis=1)
    dlow_out.start()

    wides = (wide_even, wide_odd)

    def widen(s, at):
        wides[s % 2][at, :] = stage[s % 2, at, :].astype(jnp.float32)

    for wide in wides:
        wide[pl.ds(rows, 8), :] = jnp.zeros((8, width), jnp.float32)
    fetch(1).start()
    fetch(0).wait()

    @pl.loop(0, rows // chunk)
    def _(c):
        widen(0, pl.ds(pl.multiple_of(c * chunk, chunk), chunk))

    for copy in ids_out:
        copy.wait()
    idx_in[t] = idx_ref[t]

    def peer(j):
        return (t // 2 + 1 - j // 2) % 2 * 2 + (t + (j + 1) // 2) % 2

    got_ids = [
        [
            pltpu.make_async_copy(
                idx_in.at[peer(j), pl.ds(s * maxlen, maxlen)],
                idx_s.at[s, j],
                smem_sem.at[s * owners + j],
            )
            for j in range(owners)
        ]
        for s in range(slots)
    ]
    for copies in got_ids:
        for copy in copies:
            copy.start()

    for copy in x_out + dz_out + [low_out, dlow_out]:
        copy.wait()
    low_two = jnp.concatenate([low_ref[...], low_in[...]], axis=0)
    dlow_two = jnp.concatenate([dlow_ref[...], dlow_in[...]], axis=0)
    left = lax.broadcasted_iota(jnp.int32, (half, LANES), 1) < cols
    for b in range(groups):
        at = pl.ds(pl.multiple_of(b * high + core * (high - half), 16), half)
        up = jnp.dot(
            jnp.concatenate([dzt[at, :], dz_in[b]], axis=1),
            low_two,
            preferred_element_type=jnp.float32,
        )
        down = jnp.dot(
            jnp.concatenate([xt[at, :], x_in[b]], axis=1),
            dlow_two,
            preferred_element_type=jnp.float32,
        )
        for y in range(2):
            u, d = up[:, y * LANES : (y + 1) * LANES], down[:, y * LANES : (y + 1) * LANES]
            part[y, 0, b // 4, b // 2 % 2, b % 2] = jnp.where(left, u, d).astype(jnp.bfloat16)
            part[y, 1, b // 4, b // 2 % 2, b % 2] = jnp.where(left, d, u).astype(jnp.bfloat16)

    begins = [sum(n for _, n in PLAN[:k]) * half // 14 for k in range(len(PLAN) + 1)]

    def place_of(k, held):
        span = pl.ds(begins[k], begins[k + 1] - begins[k])
        return tuple(held.get(d, slice(None)) for d in "ycvux") + (span,)

    def exchange(k, i):
        order = PLAN[k][0]
        held = {d: at_axis[d] for d in order[:i]}
        held[order[i]] = 1 - at_axis[order[i]]
        return send(
            part.at[place_of(k, held)], landing[4 * k + i], class_sem, 4 * k + i, across[order[i]]
        )

    def hand(k):
        span = pl.ds(begins[k], begins[k + 1] - begins[k])
        return send(fin_out.at[span], fin_in.at[span], fin_sem, k, mate)

    def take(k, i):
        exchange(k, i).wait()
        order, came = PLAN[k][0], landing[4 * k + i]
        held = {d: at_axis[d] for d in order[: i + 1]}
        span = pl.ds(begins[k], begins[k + 1] - begins[k])
        if i == 3:
            for c, keep in ((1 - core, False), (core, True)):
                total = part[place_of(k, held | {"c": c})].astype(jnp.float32) + came[c].astype(
                    jnp.float32
                )
                if keep:
                    fin[span, :] = total
                else:
                    fin_out[span, :] = total.astype(jnp.bfloat16)
                    hand(k).start()
            return
        free = [d for d in "ycvux" if d not in held]
        for pick in itertools.product(range(2), repeat=len(free)):
            at = place_of(k, held | dict(zip(free, pick)))
            part[at] = (part[at].astype(jnp.float32) + came[pick].astype(jnp.float32)).astype(
                jnp.bfloat16
            )
        exchange(k, i + 1).start()

    for k in range(len(PLAN)):
        if k not in dict(LATE):
            exchange(k, 0).start()

    def give(s, j):
        return send(pooled.at[j, s], got.at[t, s], pool_sem, s * (owners - 1) + j, (g, peer(j)))

    share = rows // owners
    for s in range(slots):
        for copy in got_ids[s]:
            copy.wait()
        if s + 1 < slots:
            fetch(s + 1).wait()
        if s + 2 < slots:
            fetch(s + 2).start()
        wide = wides[s % 2]

        @pl.loop(0, owners)
        def _(j):
            if s + 1 < slots:
                widen(s + 1, pl.ds(pl.multiple_of(j * share, share), share))
            ids = [idx_s.at[s, j, k] for k in range(maxlen)]
            for u in range(batch):
                held = [wide[pl.ds(ids[k][u], 1), :] for k in range(maxlen)]
                while len(held) > 1:
                    held = [a + b for a, b in zip(held[::2], held[1::2])]
                acc[pl.ds(u, 1), :] = held[0]
            pooled[j, s] = acc[...].astype(jnp.bfloat16)

            @pl.when(j < owners - 1)
            def _():
                give(s, j).start()

            for n in range(owners):
                now = s * owners + n
                todo = [p for p in POLLS if p[0] == now]
                begin = [k for k, p in LATE if p == now]
                if todo or begin:

                    @pl.when(j == n)
                    def _():
                        for _, k, i in todo:
                            take(k, i)
                        for k in begin:
                            exchange(k, 0).start()

        got[t, s] = pooled[owners - 1, s]

    for now, k, i in POLLS:
        if now >= slots * owners:
            take(k, i)
    for k in range(len(PLAN)):
        hand(k).wait()
    other = pl.ds(pl.multiple_of((1 - core) * (high - half), 16), half)
    own = pl.ds(pl.multiple_of(core * (high - half), 16), half)
    full[other, :] = fin_in[...].astype(jnp.float32)
    full[own, :] = fin[...]
    total = full[...].T
    out_ref[core] = total[:cols] * factor
    out_ref[1 - core] = total[cols:] * factor
    for s in range(slots):
        for j in range(owners - 1):
            give(s, j).wait()


def fused_step(
    next_ids, next_lengths, slot_of_table, tables, cross_input, cotangent, up_weight, down_weight, maxlen, factor
):
    groups, owners = lax.axis_size("grp"), lax.axis_size("tbl")
    slots, rows, width = tables.shape
    batch, depth = cross_input.shape
    rank = down_weight.shape[1]
    high = depth // groups
    half = (high // 2 + 15) // 16 * 16
    sems = pltpu.SemaphoreType.DMA
    bf16, f32 = jnp.bfloat16, jnp.float32
    in_hbm = pl.BlockSpec(memory_space=pltpu.HBM)
    idx_shape = (owners, next_ids.shape[1] // owners, batch)
    vmem = pl.BlockSpec(memory_space=pltpu.VMEM)
    landing = [
        pltpu.VMEM((2,) * (4 - i) + (n * half // 14, LANES), bf16)
        for _, n in PLAN
        for i in range(4)
    ]
    return pl.pallas_call(
        functools.partial(step_kernel, maxlen, factor),
        out_shape=(
            pltpu.VMEM((owners, slots, batch, width), bf16),
            pltpu.VMEM((2, rank // owners, high), f32),
        ),
        in_specs=[in_hbm] * 8,
        out_specs=(vmem, vmem),
        scratch_shapes=[
            pltpu.VMEM(next_ids.shape[::-1], jnp.int32),
            pltpu.VMEM(next_lengths.shape[::-1], jnp.int32),
            pltpu.VMEM((1, slot_of_table.shape[0]), jnp.int32),
            pltpu.VMEM(cross_input.shape, bf16),
            pltpu.VMEM(cotangent.shape, bf16),
            pltpu.VMEM(up_weight.shape, bf16),
            pltpu.VMEM(down_weight.shape, bf16),
            pltpu.VMEM((depth, batch), bf16),
            pltpu.VMEM((depth, batch), bf16),
            pltpu.VMEM((groups, half, batch), bf16),
            pltpu.VMEM((groups, half, batch), bf16),
            pltpu.VMEM((batch, rank), bf16),
            pltpu.VMEM((batch, rank), bf16),
            pltpu.VMEM((batch, rank), bf16),
            pltpu.VMEM((batch, rank), bf16),
            pltpu.VMEM(idx_shape, jnp.int32),
            pltpu.VMEM(idx_shape, jnp.int32),
            pltpu.SMEM((slots, owners, maxlen, batch), jnp.int32),
            pltpu.VMEM((2, 2, 2, 2, 2, half, LANES), bf16),
            pltpu.VMEM((half, LANES), f32),
            pltpu.VMEM((half, LANES), bf16),
            pltpu.VMEM((half, LANES), bf16),
            pltpu.VMEM((high, LANES), f32),
            pltpu.VMEM((2, rows, width), bf16),
            pltpu.VMEM((rows + 8, width), f32),
            pltpu.VMEM((rows + 8, width), f32),
            pltpu.VMEM((batch, width), f32),
            pltpu.VMEM((owners, slots, batch, width), bf16),
            sems((2,)),
            sems((slots * owners,)),
            sems((2, owners - 1)),
            sems((2, 2 * groups + 2)),
            sems((2, 4 * len(PLAN))),
            sems((2, len(PLAN))),
            sems((2, slots * (owners - 1))),
            sems((7,)),
        ]
        + landing,
        compiler_params=pltpu.CompilerParams(
            collective_id=0, has_side_effects=True, vmem_limit_bytes=48 << 20
        ),
        name="fused_step",
    )(
        *(
            pltpu.with_memory_space_constraint(a, pltpu.HBM)
            for a in (
                next_ids.T,
                next_lengths.T,
                slot_of_table[None, :],
                tables,
                cross_input,
                cotangent,
                up_weight,
                down_weight,
            )
        )
    )


def finish_kernel(slot_ref, got_ref, sum_ref, emb_ref, grad_up_ref, grad_down_ref, sem):
    slots, _, width = got_ref.shape[1:]
    feats = slot_ref.shape[0]
    copies = [
        pltpu.make_async_copy(sum_ref.at[0], grad_up_ref, sem.at[feats]),
        pltpu.make_async_copy(sum_ref.at[1], grad_down_ref, sem.at[feats + 1]),
    ]
    for f in range(feats):
        s = slot_ref[f]
        copies.append(
            pltpu.make_async_copy(
                got_ref.at[lax.div(s, slots), lax.rem(s, slots)],
                emb_ref.at[:, pl.ds(f * width, width)],
                sem.at[f],
            )
        )
    for copy in copies:
        copy.start()
    for copy in copies:
        copy.wait()


def finish(slot_of_table, got, sums):
    _, _, batch, width = got.shape
    feats = slot_of_table.shape[0]
    in_hbm = pl.BlockSpec(memory_space=pltpu.HBM)
    any_space = pl.BlockSpec(memory_space=pl.ANY)
    return pl.pallas_call(
        finish_kernel,
        out_shape=(
            jax.ShapeDtypeStruct((batch, feats * width), jnp.bfloat16),
            jax.ShapeDtypeStruct(sums.shape[1:], jnp.float32),
            jax.ShapeDtypeStruct(sums.shape[1:], jnp.float32),
        ),
        in_specs=[pl.BlockSpec(memory_space=pltpu.SMEM), any_space, any_space],
        out_specs=(in_hbm, in_hbm, in_hbm),
        scratch_shapes=[pltpu.SemaphoreType.DMA((feats + 2,))],
        compiler_params=pltpu.CompilerParams(vmem_limit_bytes=1 << 20),
        name="finish",
    )(slot_of_table, got, sums)


def on_device(
    next_ids, next_lengths, slot_of_table, tables, cross_input, cotangent, up_weight, down_weight
):
    groups, owners = lax.axis_size("grp"), lax.axis_size("tbl")
    batch, depth = cross_input.shape
    rank = down_weight.shape[1]
    slots, rows, _ = tables.shape
    maxlen = next_ids.shape[1] // (slots * owners)
    fits = (
        owners == 4
        and groups == 8
        and depth % (16 * groups) == 0
        and depth % LANES == 0
        and depth // groups <= 448
        and depth // groups > 432 - 16
        and rank == 256
        and maxlen == 8
        and slots > 2
        and rows % 1024 == 0
        and batch == LANES
    )
    args = (
        next_ids,
        next_lengths,
        slot_of_table,
        tables,
        cross_input,
        cotangent,
        up_weight,
        down_weight,
    )
    if not fits:
        return plain(*args)
    factor = 1.0 / math.sqrt(batch * groups * owners)
    got, sums = fused_step(*args, maxlen, factor)
    next_embedded, grad_up, grad_down = finish(slot_of_table, got, sums)
    return next_embedded, grad_up, grad_down.T


def solution(mesh):
    return jax.shard_map(
        on_device,
        mesh=mesh,
        in_specs=(
            P(("grp", "tbl"), None),
            P(("grp", "tbl"), None),
            P(),
            P("tbl", None, None),
            P(("grp", "tbl"), None),
            P(("grp", "tbl"), None),
            P(),
            P(),
        ),
        out_specs=(P(("grp", "tbl"), None), P("tbl", "grp"), P("grp", "tbl")),
        check_vma=False,
    )
```

```python
import functools
import itertools
import math

import jax
import jax.numpy as jnp
from jax import lax
from jax.experimental import pallas as pl
from jax.experimental.pallas import tpu as pltpu
from jax.sharding import PartitionSpec as P

LANES = 128


def pool_kernel(maxlen, idx_ref, tab_ref, out_ref, stage, wide, acc, sem):
    owners, batch, _ = out_ref.shape
    slots, rows, width = tab_ref.shape
    per_line = LANES // maxlen
    lines = batch // per_line
    chunk = 256

    def fetch(s):
        return pltpu.make_async_copy(tab_ref.at[s], stage.at[s % 2], sem.at[s % 2])

    fetch(0).start()
    wide[pl.ds(rows, 8), :] = jnp.zeros((8, width), jnp.float32)
    for s in range(slots):
        if s + 1 < slots:
            fetch(s + 1).start()
        fetch(s).wait()

        @pl.loop(0, rows // chunk)
        def _(c):
            at = pl.ds(pl.multiple_of(c * chunk, chunk), chunk)
            wide[at, :] = stage[s % 2, at, :].astype(jnp.float32)

        @pl.loop(0, owners * lines)
        def _(g):
            src = g // lines
            line = s * lines + g % lines
            for u in range(per_line):
                got = [
                    wide[pl.ds(idx_ref[src, line, u * maxlen + k], 1), :] for k in range(maxlen)
                ]
                while len(got) > 1:
                    got = [a + b for a, b in zip(got[::2], got[1::2])] + (
                        [got[-1]] if len(got) % 2 else []
                    )
                acc[pl.ds(g * per_line + u, 1), :] = got[0]

        for o in range(owners):
            out_ref[o, :, s * width : (s + 1) * width] = acc[
                o * batch : (o + 1) * batch, :
            ].astype(jnp.bfloat16)


def pool(idx, tables, batch, maxlen):
    slots, rows, width = tables.shape
    owners = idx.shape[0]
    return pl.pallas_call(
        functools.partial(pool_kernel, maxlen),
        out_shape=jax.ShapeDtypeStruct((owners, batch, slots * width), jnp.bfloat16),
        in_specs=[
            pl.BlockSpec(memory_space=pltpu.SMEM),
            pl.BlockSpec(memory_space=pl.ANY),
        ],
        out_specs=pl.BlockSpec(memory_space=pltpu.VMEM),
        scratch_shapes=[
            pltpu.VMEM((2, rows, width), jnp.bfloat16),
            pltpu.VMEM((rows + 8, width), jnp.float32),
            pltpu.VMEM((owners * batch, width), jnp.float32),
            pltpu.SemaphoreType.DMA((2,)),
        ],
        compiler_params=pltpu.CompilerParams(vmem_limit_bytes=60 << 20),
        cost_estimate=pl.CostEstimate(
            flops=100_000_000, bytes_accessed=tables.size * 2, transcendentals=0
        ),
        name="pool",
    )(idx, tables)


def order_kernel(slot_ref, got_ref, out_ref):
    owners, batch, wide = got_ref.shape
    feats = slot_ref.shape[0]
    width = out_ref.shape[1] // feats
    slots = wide // width
    for f in range(feats):
        s = slot_ref[f]
        at = pl.ds(pl.multiple_of(lax.rem(s, slots) * width, width), width)
        out_ref[:, f * width : (f + 1) * width] = got_ref[lax.div(s, slots), :, at]


def order(slot_of_table, got, width):
    return pl.pallas_call(
        order_kernel,
        out_shape=jax.ShapeDtypeStruct(
            (got.shape[1], slot_of_table.shape[0] * width), jnp.bfloat16
        ),
        in_specs=[
            pl.BlockSpec(memory_space=pltpu.SMEM),
            pl.BlockSpec(memory_space=pltpu.VMEM),
        ],
        out_specs=pl.BlockSpec(memory_space=pltpu.VMEM),
        name="order",
    )(slot_of_table, got)


def bag_rows(next_ids, next_lengths, slot_of_table, slots, owners, rows):
    batch = next_ids.shape[0]
    slots_all = slots * owners
    maxlen = next_ids.shape[1] // slots_all
    hit = (slot_of_table[:, None] == lax.broadcasted_iota(jnp.int32, (1, slots_all), 1)).astype(
        jnp.int32
    )
    slot_lengths = jnp.sum(next_lengths[:, :, None] * hit[None, :, :], axis=1)
    keep = lax.broadcasted_iota(jnp.int32, (batch, slots_all, maxlen), 2) < slot_lengths[:, :, None]
    idx = jnp.where(keep, next_ids.reshape(batch, slots_all, maxlen), rows)
    return idx.transpose(1, 0, 2).reshape(owners, slots * batch * maxlen // LANES, LANES)


def plain(
    next_ids, next_lengths, slot_of_table, tables, cross_input, cotangent, up_weight, down_weight
):
    batch = next_ids.shape[0]
    owners = lax.axis_size("tbl")
    slots, rows, width = tables.shape
    maxlen = next_ids.shape[1] // (slots * owners)
    idx = bag_rows(next_ids, next_lengths, slot_of_table, slots, owners, rows)
    low = jnp.dot(cross_input, down_weight, preferred_element_type=jnp.float32).astype(jnp.bfloat16)
    dz = (cotangent.astype(jnp.float32) * cross_input.astype(jnp.float32)).astype(jnp.bfloat16)
    dlow = jnp.dot(dz, up_weight.T, preferred_element_type=jnp.float32).astype(jnp.bfloat16)
    total = batch * lax.axis_size("grp") * owners
    factor = 1.0 / math.sqrt(total)
    part_up = jnp.dot(low.T, dz, preferred_element_type=jnp.float32) * factor
    part_down = jnp.dot(cross_input.T, dlow, preferred_element_type=jnp.float32) * factor
    part_up, part_down = part_up.astype(jnp.bfloat16), part_down.astype(jnp.bfloat16)
    owner_up, owner_down = (
        lax.psum_scatter(part_up, "tbl", scatter_dimension=0, tiled=True).astype(jnp.float32),
        lax.psum_scatter(part_down, "tbl", scatter_dimension=1, tiled=True).astype(jnp.float32),
    )
    got_idx = lax.all_to_all(idx, "tbl", split_axis=0, concat_axis=0, tiled=True)
    pooled = pool(got_idx, tables, batch, maxlen)
    returned = lax.all_to_all(pooled, "tbl", split_axis=0, concat_axis=0, tiled=True)
    next_embedded = order(slot_of_table, returned, width)
    grad_up, grad_down = (
        lax.psum_scatter(owner_up, "grp", scatter_dimension=1, tiled=True),
        lax.psum_scatter(owner_down, "grp", scatter_dimension=0, tiled=True),
    )
    return (next_embedded, grad_up, grad_down)


PLAN = (("uxyv", 5), ("yuxv", 3), ("xyuv", 2), ("xuvy", 4))
POLLS = ((12, 3, 0), (13, 0, 0), (15, 2, 0), (15, 1, 0), (21, 3, 1), (22, 2, 1), (23, 1, 1), (23, 0, 1), (28, 1, 2), (28, 2, 2), (28, 0, 2), (28, 3, 2), (28, 2, 3), (28, 3, 3), (28, 1, 3), (28, 0, 3))
LATE = ((2, 7),)


def step_kernel(
    maxlen,
    factor,
    ids_hbm,
    len_hbm,
    slot_hbm,
    tab_ref,
    x_hbm,
    ct_hbm,
    up_hbm,
    down_hbm,
    emb_ref,
    out_ref,
    ids_ref,
    len_ref,
    slot_ref,
    slot_s,
    x_ref,
    ct_ref,
    up_ref,
    down_ref,
    xt,
    dzt,
    x_in,
    dz_in,
    low_ref,
    dlow_ref,
    low_in,
    dlow_in,
    idx_ref,
    idx_in,
    idx_s,
    rise,
    part,
    full,
    stage,
    wide_even,
    wide_odd,
    acc,
    pooled,
    got,
    tab_sem,
    smem_sem,
    idx_sem,
    mate_sem,
    class_sem,
    fin_sem,
    pool_sem,
    load_sem,
    *landing,
):
    slots, rows, width = tab_ref.shape
    batch, depth = x_ref.shape
    rank = down_ref.shape[1]
    half = x_in.shape[1]
    owners, groups = 4, 8
    high = depth // groups
    cols = rank // owners
    chunk = 1024
    g, t = lax.axis_index("grp"), lax.axis_index("tbl")
    core = t % 2
    at_axis = {"y": t // 2, "v": g // 4, "u": g // 2 % 2, "x": g % 2}
    mate = (g, t + 1 - 2 * core)
    across = {
        "y": (g, (t + 2) % owners),
        "v": ((g + 4) % groups, t),
        "u": (g + 2 - 4 * at_axis["u"], t),
        "x": (g + 1 - 2 * at_axis["x"], t),
    }

    def fetch(s):
        return pltpu.make_async_copy(tab_ref.at[s], stage.at[s % 2], tab_sem.at[s % 2])

    def send(src, dst, sems, n, device):
        return pltpu.make_async_remote_copy(
            src_ref=src,
            dst_ref=dst,
            send_sem=sems.at[0, n],
            recv_sem=sems.at[1, n],
            device_id=device,
            device_id_type=pl.DeviceIdType.MESH,
        )

    loads = [
        pltpu.make_async_copy(a, b, load_sem.at[n])
        for n, (a, b) in enumerate(
            (
                (ids_hbm, ids_ref),
                (len_hbm, len_ref),
                (slot_hbm, slot_ref),
                (x_hbm, x_ref),
                (ct_hbm, ct_ref),
                (down_hbm, down_ref),
                (up_hbm, up_ref),
                (slot_hbm, slot_s),
            )
        )
    ]
    for copy in loads:
        copy.start()
    fetch(0).start()
    fetch(1).start()
    barrier = pltpu.get_barrier_semaphore()
    beside = {d: (a, b + 1 - 2 * core) for d, (a, b) in across.items()}
    near = [(g, (t + d) % owners) for d in range(1, owners)] + [across[d] for d in "vux"]
    near += [beside[d] for d in "vux" if any(order[3] == d for order, _ in PLAN)]
    for device in near:
        pl.semaphore_signal(
            barrier, inc=1, device_id=device, device_id_type=pl.DeviceIdType.MESH
        )

    for copy in loads[:3]:
        copy.wait()
    feats, span = slot_ref.shape[1], ids_ref.shape[0]
    each = slots * maxlen
    entry = lax.broadcasted_iota(jnp.int32, (span, feats), 0)
    hit = jnp.where(slot_ref[...] == entry // maxlen, 1.0, 0.0).astype(jnp.bfloat16)
    lens = jnp.dot(
        hit, len_ref[...].astype(jnp.float32).astype(jnp.bfloat16), preferred_element_type=jnp.float32
    )
    place = (lax.broadcasted_iota(jnp.int32, (span, batch), 0) % maxlen).astype(jnp.float32)
    idx = jnp.where(place < lens, ids_ref[...], rows)
    for o in range(owners):
        idx_ref[o] = idx[o * each : (o + 1) * each]

    def turn(src, dst):
        for n in range(depth // LANES):
            at = slice(n * LANES, (n + 1) * LANES)
            dst[at, :] = src[:, at].T

    ids_out = [
        send(idx_ref.at[(t + d) % owners], idx_in.at[t], idx_sem, d - 1, (g, (t + d) % owners))
        for d in range(1, owners)
    ]

    def lend(src, dst, n):
        return [
            send(
                src.at[pl.ds(pl.multiple_of(b * high + (1 - core) * (high - half), 16), half)],
                dst.at[b],
                mate_sem,
                n + b,
                mate,
            )
            for b in range(groups)
        ]

    x_out, dz_out = lend(xt, x_in, 0), lend(dzt, dz_in, groups)
    low_out = send(low_ref, low_in, mate_sem, 2 * groups, mate)
    dlow_out = send(dlow_ref, dlow_in, mate_sem, 2 * groups + 1, mate)
    for wide in (wide_even, wide_odd):
        wide[pl.ds(rows, 8), :] = jnp.zeros((8, width), jnp.float32)
    loads[3].wait()
    turn(x_ref, xt)
    pl.semaphore_wait(barrier, len(near))
    for copy in ids_out + x_out:
        copy.start()
    loads[4].wait()
    ct_ref[...] = (ct_ref[...].astype(jnp.float32) * x_ref[...].astype(jnp.float32)).astype(
        jnp.bfloat16
    )
    turn(ct_ref, dzt)
    for copy in dz_out:
        copy.start()
    loads[5].wait()
    low_ref[...] = jnp.dot(
        x_ref[...], down_ref[...], preferred_element_type=jnp.float32
    ).astype(jnp.bfloat16)
    low_out.start()
    loads[6].wait()
    dlow = jnp.dot(up_ref[...], dzt[...], preferred_element_type=jnp.float32).astype(jnp.bfloat16).T
    swap = [n + 1 - 2 * (n % 2) for n in range(owners)]
    dlow_ref[...] = jnp.concatenate([dlow[:, n * cols : (n + 1) * cols] for n in swap], axis=1)
    dlow_out.start()

    wides = (wide_even, wide_odd)

    def widen(s, at):
        wides[s % 2][at, :] = stage[s % 2, at, :].astype(jnp.float32)

    fetch(0).wait()

    @pl.loop(0, rows // chunk)
    def _(c):
        widen(0, pl.ds(pl.multiple_of(c * chunk, chunk), chunk))

    def peer(j):
        return (t // 2 + 1 - j // 2) % 2 * 2 + (t + (j + 1) // 2) % 2

    got_ids = [
        [
            pltpu.make_async_copy(
                idx_in.at[peer(j), pl.ds(s * maxlen, maxlen)],
                idx_s.at[s, j],
                smem_sem.at[s * owners + j],
            )
            for j in range(owners)
        ]
        for s in range(slots)
    ]
    for copy in ids_out:
        copy.wait()
    idx_in[t] = idx_ref[t]
    for copies in got_ids:
        for copy in copies:
            copy.start()
    for copy in dz_out + [low_out]:
        copy.wait()
    rises = [
        pl.ds(pl.multiple_of(b * high + core * (high - half), 16), half) for b in range(groups)
    ]
    low_two = jnp.concatenate([low_ref[...], low_in[...]], axis=0)
    for b in range(groups):
        both = jnp.concatenate([dzt[rises[b], :], dz_in[b]], axis=1)
        rise[b] = jnp.dot(both, low_two, preferred_element_type=jnp.float32).astype(jnp.bfloat16)
    for copy in x_out + [dlow_out]:
        copy.wait()
    dlow_two = jnp.concatenate([dlow_ref[...], dlow_in[...]], axis=0)
    left = lax.broadcasted_iota(jnp.int32, (half, LANES), 1) < cols
    for b in range(groups):
        both = jnp.concatenate([xt[rises[b], :], x_in[b]], axis=1)
        down = jnp.dot(both, dlow_two, preferred_element_type=jnp.float32).astype(jnp.bfloat16)
        for y in range(2):
            u, d = rise[b, :, y * LANES : (y + 1) * LANES], down[:, y * LANES : (y + 1) * LANES]
            part[y, 0, b // 4, b // 2 % 2, b % 2] = jnp.where(left, u, d)
            part[y, 1, b // 4, b // 2 % 2, b % 2] = jnp.where(left, d, u)

    begins = [sum(n for _, n in PLAN[:k]) * half // 14 for k in range(len(PLAN) + 1)]

    def place_of(k, held):
        span = pl.ds(begins[k], begins[k + 1] - begins[k])
        return tuple(held.get(d, slice(None)) for d in "ycvux") + (span,)

    def exchange(k, i):
        order = PLAN[k][0]
        held = {d: at_axis[d] for d in order[:i]}
        held[order[i]] = 1 - at_axis[order[i]]
        return send(
            part.at[place_of(k, held)], landing[4 * k + i], class_sem, 4 * k + i, across[order[i]]
        )

    def last(k):
        order = PLAN[k][0]
        d = order[3]
        held = {e: at_axis[e] for e in order}
        there, here = held | {d: 1 - at_axis[d]}, held
        return [
            send(
                part.at[place_of(k, there | {"c": core})],
                landing[4 * k + 3].at[0],
                class_sem,
                4 * k + 3,
                across[d],
            ),
            send(
                part.at[place_of(k, there | {"c": 1 - core})],
                landing[4 * k + 3].at[1],
                fin_sem,
                2 * k,
                beside[d],
            ),
            send(
                part.at[place_of(k, here | {"c": 1 - core})],
                landing[4 * k + 3].at[2],
                fin_sem,
                2 * k + 1,
                mate,
            ),
        ]

    def take(k, i):
        order, came = PLAN[k][0], landing[4 * k + i]
        held = {d: at_axis[d] for d in order[: i + 1]}
        if i == 3:
            for copy in last(k):
                copy.wait()
            size = begins[k + 1] - begins[k]
            other = pl.ds(pl.multiple_of((1 - core) * (high - half) + begins[k], 16), size)
            own = pl.ds(pl.multiple_of(core * (high - half) + begins[k], 16), size)
            mine = part[place_of(k, held | {"c": core})].astype(jnp.float32)
            full[other, :] = came[1].astype(jnp.float32) + came[2].astype(jnp.float32)
            full[own, :] = mine + came[0].astype(jnp.float32)
            return
        exchange(k, i).wait()
        free = [d for d in "ycvux" if d not in held]
        for pick in itertools.product(range(2), repeat=len(free)):
            at = place_of(k, held | dict(zip(free, pick)))
            part[at] = (part[at].astype(jnp.float32) + came[pick].astype(jnp.float32)).astype(
                jnp.bfloat16
            )
        if i == 2:
            for copy in last(k):
                copy.start()
        else:
            exchange(k, i + 1).start()

    for k in range(len(PLAN)):
        if k not in dict(LATE):
            exchange(k, 0).start()

    def give(s, j):
        return send(pooled.at[j, s], got.at[t, s], pool_sem, s * (owners - 1) + j, (g, peer(j)))

    share = rows // owners
    for s in range(slots):
        for copy in got_ids[s]:
            copy.wait()
        if s + 1 < slots:
            fetch(s + 1).wait()
        if s + 2 < slots:
            fetch(s + 2).start()
        wide = wides[s % 2]

        @pl.loop(0, owners)
        def _(j):
            if s + 1 < slots:
                widen(s + 1, pl.ds(pl.multiple_of(j * share, share), share))
            ids = [idx_s.at[s, j, k] for k in range(maxlen)]
            for u in range(batch):
                held = [wide[pl.ds(ids[k][u], 1), :] for k in range(maxlen)]
                while len(held) > 1:
                    held = [a + b for a, b in zip(held[::2], held[1::2])]
                acc[pl.ds(u, 1), :] = held[0]
            pooled[j, s] = acc[...].astype(jnp.bfloat16)

            @pl.when(j < owners - 1)
            def _():
                give(s, j).start()

            for n in range(owners):
                now = s * owners + n
                todo = [p for p in POLLS if p[0] == now]
                begin = [k for k, p in LATE if p == now]
                if todo or begin:

                    @pl.when(j == n)
                    def _():
                        for _, k, i in todo:
                            take(k, i)
                        for k in begin:
                            exchange(k, 0).start()

        got[t, s] = pooled[owners - 1, s]

    tail = [(k, i) for now, k, i in POLLS if now >= slots * owners]
    for n, (k, i) in enumerate(tail):
        if all(i == 3 for _, i in tail[n:]) and tail[n - 1][1] < 3:
            for s in range(slots):
                for j in range(owners - 1):
                    give(s, j).wait()
            loads[7].wait()
            for f in range(feats):
                s = slot_s[0, f]
                emb_ref[:, f * width : (f + 1) * width] = got[lax.div(s, slots), lax.rem(s, slots)]
        take(k, i)
    total = full[...].T
    out_ref[core] = total[:cols] * factor
    out_ref[1 - core] = total[cols:] * factor


def fused_step(
    next_ids, next_lengths, slot_of_table, tables, cross_input, cotangent, up_weight, down_weight, maxlen, factor
):
    groups, owners = lax.axis_size("grp"), lax.axis_size("tbl")
    slots, rows, width = tables.shape
    batch, depth = cross_input.shape
    rank = down_weight.shape[1]
    high = depth // groups
    half = (high // 2 + 15) // 16 * 16
    sems = pltpu.SemaphoreType.DMA
    bf16, f32 = jnp.bfloat16, jnp.float32
    in_hbm = pl.BlockSpec(memory_space=pltpu.HBM)
    idx_shape = (owners, next_ids.shape[1] // owners, batch)
    vmem = pl.BlockSpec(memory_space=pltpu.VMEM)
    landing = [
        pltpu.VMEM(((2,) * (4 - i) if i < 3 else (3,)) + (n * half // 14, LANES), bf16)
        for _, n in PLAN
        for i in range(4)
    ]
    return pl.pallas_call(
        functools.partial(step_kernel, maxlen, factor),
        out_shape=(
            pltpu.VMEM((batch, slot_of_table.shape[0] * width), bf16),
            pltpu.VMEM((2, rank // owners, high), f32),
        ),
        in_specs=[in_hbm] * 8,
        out_specs=(vmem, vmem),
        scratch_shapes=[
            pltpu.VMEM(next_ids.shape[::-1], jnp.int32),
            pltpu.VMEM(next_lengths.shape[::-1], jnp.int32),
            pltpu.VMEM((1, slot_of_table.shape[0]), jnp.int32),
            pltpu.SMEM((1, slot_of_table.shape[0]), jnp.int32),
            pltpu.VMEM(cross_input.shape, bf16),
            pltpu.VMEM(cotangent.shape, bf16),
            pltpu.VMEM(up_weight.shape, bf16),
            pltpu.VMEM(down_weight.shape, bf16),
            pltpu.VMEM((depth, batch), bf16),
            pltpu.VMEM((depth, batch), bf16),
            pltpu.VMEM((groups, half, batch), bf16),
            pltpu.VMEM((groups, half, batch), bf16),
            pltpu.VMEM((batch, rank), bf16),
            pltpu.VMEM((batch, rank), bf16),
            pltpu.VMEM((batch, rank), bf16),
            pltpu.VMEM((batch, rank), bf16),
            pltpu.VMEM(idx_shape, jnp.int32),
            pltpu.VMEM(idx_shape, jnp.int32),
            pltpu.SMEM((slots, owners, maxlen, batch), jnp.int32),
            pltpu.VMEM((groups, half, rank), bf16),
            pltpu.VMEM((2, 2, 2, 2, 2, half, LANES), bf16),
            pltpu.VMEM((high, LANES), f32),
            pltpu.VMEM((2, rows, width), bf16),
            pltpu.VMEM((rows + 8, width), f32),
            pltpu.VMEM((rows + 8, width), f32),
            pltpu.VMEM((batch, width), f32),
            pltpu.VMEM((owners, slots, batch, width), bf16),
            pltpu.VMEM((owners, slots, batch, width), bf16),
            sems((2,)),
            sems((slots * owners,)),
            sems((2, owners - 1)),
            sems((2, 2 * groups + 2)),
            sems((2, 4 * len(PLAN))),
            sems((2, 2 * len(PLAN))),
            sems((2, slots * (owners - 1))),
            sems((8,)),
        ]
        + landing,
        compiler_params=pltpu.CompilerParams(
            collective_id=0, has_side_effects=True, vmem_limit_bytes=48 << 20
        ),
        name="fused_step",
    )(
        *(
            pltpu.with_memory_space_constraint(a, pltpu.HBM)
            for a in (
                next_ids.T,
                next_lengths.T,
                slot_of_table[None, :],
                tables,
                cross_input,
                cotangent,
                up_weight,
                down_weight,
            )
        )
    )


def finish_kernel(emb_in, sum_in, emb_ref, grad_up_ref, grad_down_ref, sem):
    copies = [
        pltpu.make_async_copy(a, b, sem.at[n])
        for n, (a, b) in enumerate(
            ((emb_in, emb_ref), (sum_in.at[0], grad_up_ref), (sum_in.at[1], grad_down_ref))
        )
    ]
    for copy in copies:
        copy.start()
    for copy in copies:
        copy.wait()


def finish(emb, sums):
    in_hbm = pl.BlockSpec(memory_space=pltpu.HBM)
    any_space = pl.BlockSpec(memory_space=pl.ANY)
    return pl.pallas_call(
        finish_kernel,
        out_shape=(
            jax.ShapeDtypeStruct(emb.shape, emb.dtype),
            jax.ShapeDtypeStruct(sums.shape[1:], jnp.float32),
            jax.ShapeDtypeStruct(sums.shape[1:], jnp.float32),
        ),
        in_specs=[any_space, any_space],
        out_specs=(in_hbm, in_hbm, in_hbm),
        scratch_shapes=[pltpu.SemaphoreType.DMA((3,))],
        compiler_params=pltpu.CompilerParams(vmem_limit_bytes=1 << 20),
        name="finish",
    )(emb, sums)


def on_device(
    next_ids, next_lengths, slot_of_table, tables, cross_input, cotangent, up_weight, down_weight
):
    groups, owners = lax.axis_size("grp"), lax.axis_size("tbl")
    batch, depth = cross_input.shape
    rank = down_weight.shape[1]
    slots, rows, _ = tables.shape
    maxlen = next_ids.shape[1] // (slots * owners)
    fits = (
        owners == 4
        and groups == 8
        and depth % (16 * groups) == 0
        and depth % LANES == 0
        and depth // groups <= 448
        and depth // groups > 432 - 16
        and rank == 256
        and maxlen == 8
        and slots > 2
        and rows % 1024 == 0
        and batch == LANES
    )
    args = (
        next_ids,
        next_lengths,
        slot_of_table,
        tables,
        cross_input,
        cotangent,
        up_weight,
        down_weight,
    )
    if not fits:
        return plain(*args)
    factor = 1.0 / math.sqrt(batch * groups * owners)
    next_embedded, grad_up, grad_down = finish(*fused_step(*args, maxlen, factor))
    return next_embedded, grad_up, grad_down.T


def solution(mesh):
    return jax.shard_map(
        on_device,
        mesh=mesh,
        in_specs=(
            P(("grp", "tbl"), None),
            P(("grp", "tbl"), None),
            P(),
            P("tbl", None, None),
            P(("grp", "tbl"), None),
            P(("grp", "tbl"), None),
            P(),
            P(),
        ),
        out_specs=(P(("grp", "tbl"), None), P("tbl", "grp"), P("grp", "tbl")),
        check_vma=False,
    )
```

```python
import functools
import itertools
import math

import jax
import jax.numpy as jnp
from jax import lax
from jax.experimental import pallas as pl
from jax.experimental.pallas import tpu as pltpu
from jax.sharding import PartitionSpec as P

LANES = 128


def pool_kernel(maxlen, idx_ref, tab_ref, out_ref, stage, wide, acc, sem):
    owners, batch, _ = out_ref.shape
    slots, rows, width = tab_ref.shape
    per_line = LANES // maxlen
    lines = batch // per_line
    chunk = 256

    def fetch(s):
        return pltpu.make_async_copy(tab_ref.at[s], stage.at[s % 2], sem.at[s % 2])

    fetch(0).start()
    wide[pl.ds(rows, 8), :] = jnp.zeros((8, width), jnp.float32)
    for s in range(slots):
        if s + 1 < slots:
            fetch(s + 1).start()
        fetch(s).wait()

        @pl.loop(0, rows // chunk)
        def _(c):
            at = pl.ds(pl.multiple_of(c * chunk, chunk), chunk)
            wide[at, :] = stage[s % 2, at, :].astype(jnp.float32)

        @pl.loop(0, owners * lines)
        def _(g):
            src = g // lines
            line = s * lines + g % lines
            for u in range(per_line):
                got = [
                    wide[pl.ds(idx_ref[src, line, u * maxlen + k], 1), :] for k in range(maxlen)
                ]
                while len(got) > 1:
                    got = [a + b for a, b in zip(got[::2], got[1::2])] + (
                        [got[-1]] if len(got) % 2 else []
                    )
                acc[pl.ds(g * per_line + u, 1), :] = got[0]

        for o in range(owners):
            out_ref[o, :, s * width : (s + 1) * width] = acc[
                o * batch : (o + 1) * batch, :
            ].astype(jnp.bfloat16)


def pool(idx, tables, batch, maxlen):
    slots, rows, width = tables.shape
    owners = idx.shape[0]
    return pl.pallas_call(
        functools.partial(pool_kernel, maxlen),
        out_shape=jax.ShapeDtypeStruct((owners, batch, slots * width), jnp.bfloat16),
        in_specs=[
            pl.BlockSpec(memory_space=pltpu.SMEM),
            pl.BlockSpec(memory_space=pl.ANY),
        ],
        out_specs=pl.BlockSpec(memory_space=pltpu.VMEM),
        scratch_shapes=[
            pltpu.VMEM((2, rows, width), jnp.bfloat16),
            pltpu.VMEM((rows + 8, width), jnp.float32),
            pltpu.VMEM((owners * batch, width), jnp.float32),
            pltpu.SemaphoreType.DMA((2,)),
        ],
        compiler_params=pltpu.CompilerParams(vmem_limit_bytes=60 << 20),
        cost_estimate=pl.CostEstimate(
            flops=100_000_000, bytes_accessed=tables.size * 2, transcendentals=0
        ),
        name="pool",
    )(idx, tables)


def order_kernel(slot_ref, got_ref, out_ref):
    owners, batch, wide = got_ref.shape
    feats = slot_ref.shape[0]
    width = out_ref.shape[1] // feats
    slots = wide // width
    for f in range(feats):
        s = slot_ref[f]
        at = pl.ds(pl.multiple_of(lax.rem(s, slots) * width, width), width)
        out_ref[:, f * width : (f + 1) * width] = got_ref[lax.div(s, slots), :, at]


def order(slot_of_table, got, width):
    return pl.pallas_call(
        order_kernel,
        out_shape=jax.ShapeDtypeStruct(
            (got.shape[1], slot_of_table.shape[0] * width), jnp.bfloat16
        ),
        in_specs=[
            pl.BlockSpec(memory_space=pltpu.SMEM),
            pl.BlockSpec(memory_space=pltpu.VMEM),
        ],
        out_specs=pl.BlockSpec(memory_space=pltpu.VMEM),
        name="order",
    )(slot_of_table, got)


def bag_rows(next_ids, next_lengths, slot_of_table, slots, owners, rows):
    batch = next_ids.shape[0]
    slots_all = slots * owners
    maxlen = next_ids.shape[1] // slots_all
    hit = (slot_of_table[:, None] == lax.broadcasted_iota(jnp.int32, (1, slots_all), 1)).astype(
        jnp.int32
    )
    slot_lengths = jnp.sum(next_lengths[:, :, None] * hit[None, :, :], axis=1)
    keep = lax.broadcasted_iota(jnp.int32, (batch, slots_all, maxlen), 2) < slot_lengths[:, :, None]
    idx = jnp.where(keep, next_ids.reshape(batch, slots_all, maxlen), rows)
    return idx.transpose(1, 0, 2).reshape(owners, slots * batch * maxlen // LANES, LANES)


def plain(
    next_ids, next_lengths, slot_of_table, tables, cross_input, cotangent, up_weight, down_weight
):
    batch = next_ids.shape[0]
    owners = lax.axis_size("tbl")
    slots, rows, width = tables.shape
    maxlen = next_ids.shape[1] // (slots * owners)
    idx = bag_rows(next_ids, next_lengths, slot_of_table, slots, owners, rows)
    low = jnp.dot(cross_input, down_weight, preferred_element_type=jnp.float32).astype(jnp.bfloat16)
    dz = (cotangent.astype(jnp.float32) * cross_input.astype(jnp.float32)).astype(jnp.bfloat16)
    dlow = jnp.dot(dz, up_weight.T, preferred_element_type=jnp.float32).astype(jnp.bfloat16)
    total = batch * lax.axis_size("grp") * owners
    factor = 1.0 / math.sqrt(total)
    part_up = jnp.dot(low.T, dz, preferred_element_type=jnp.float32) * factor
    part_down = jnp.dot(cross_input.T, dlow, preferred_element_type=jnp.float32) * factor
    part_up, part_down = part_up.astype(jnp.bfloat16), part_down.astype(jnp.bfloat16)
    owner_up, owner_down = (
        lax.psum_scatter(part_up, "tbl", scatter_dimension=0, tiled=True).astype(jnp.float32),
        lax.psum_scatter(part_down, "tbl", scatter_dimension=1, tiled=True).astype(jnp.float32),
    )
    got_idx = lax.all_to_all(idx, "tbl", split_axis=0, concat_axis=0, tiled=True)
    pooled = pool(got_idx, tables, batch, maxlen)
    returned = lax.all_to_all(pooled, "tbl", split_axis=0, concat_axis=0, tiled=True)
    next_embedded = order(slot_of_table, returned, width)
    grad_up, grad_down = (
        lax.psum_scatter(owner_up, "grp", scatter_dimension=1, tiled=True),
        lax.psum_scatter(owner_down, "grp", scatter_dimension=0, tiled=True),
    )
    return (next_embedded, grad_up, grad_down)


PLAN = (("uxy", "v", 3), ("xy", "vu", 2), ("vux", "y", 3), ("xuv", "y", 4), ("yxu", "v", 2))
POLLS = ((11, 3, 0), (13, 4, 0), (15, 0, 0), (16, 2, 0), (18, 1, 0), (19, 4, 1), (19, 3, 1), (22, 0, 1), (24, 1, 1), (25, 4, 2), (25, 2, 1), (28, 0, 2), (28, 3, 2), (28, 2, 2), (28, 4, 3), (28, 1, 2), (28, 3, 3), (28, 0, 3), (28, 2, 3))
LATE = ((1, 8), (4, 1))
SORT = 3


def flips(final):
    return ["".join(p) for n in range(1, len(final) + 1) for p in itertools.combinations(final, n)]


def step_kernel(
    maxlen,
    factor,
    ids_hbm,
    len_hbm,
    slot_hbm,
    tab_ref,
    x_hbm,
    ct_hbm,
    up_hbm,
    down_hbm,
    emb_ref,
    out_ref,
    ids_ref,
    len_ref,
    slot_ref,
    slot_s,
    x_ref,
    ct_ref,
    up_ref,
    down_ref,
    xt,
    dzt,
    x_in,
    dz_in,
    low_ref,
    dlow_ref,
    low_in,
    dlow_in,
    idx_ref,
    idx_in,
    idx_s,
    rise,
    part,
    full,
    stage,
    wide_even,
    wide_odd,
    acc,
    pooled,
    got,
    tab_sem,
    smem_sem,
    idx_sem,
    mate_sem,
    step_sem,
    pool_sem,
    load_sem,
    *landing,
):
    slots, rows, width = tab_ref.shape
    batch, depth = x_ref.shape
    rank = down_ref.shape[1]
    half = x_in.shape[1]
    owners, groups = 4, 8
    high = depth // groups
    cols = rank // owners
    chunk = 1024
    g, t = lax.axis_index("grp"), lax.axis_index("tbl")
    core = t % 2
    at_axis = {"y": t // 2, "v": g // 4, "u": g // 2 % 2, "x": g % 2}

    def device(flip, turned=False):
        at = {d: 1 - v if d in flip else v for d, v in at_axis.items()}
        c = 1 - core if turned else core
        return at["v"] * 4 + at["u"] * 2 + at["x"], at["y"] * 2 + c

    mate = device("", True)
    meets = {("y", False), ("y", True), ("", True)}
    for head, final, _ in PLAN:
        meets |= {(d, False) for d in head}
        meets |= {(flip, c) for flip in flips(final) for c in (False, True)}

    def fetch(s):
        return pltpu.make_async_copy(tab_ref.at[s], stage.at[s % 2], tab_sem.at[s % 2])

    def send(src, dst, out_sem, in_sem, who):
        return pltpu.make_async_remote_copy(
            src_ref=src,
            dst_ref=dst,
            send_sem=out_sem,
            recv_sem=in_sem,
            device_id=who,
            device_id_type=pl.DeviceIdType.MESH,
        )

    loads = [
        pltpu.make_async_copy(a, b, load_sem.at[n])
        for n, (a, b) in enumerate(
            (
                (ids_hbm, ids_ref),
                (len_hbm, len_ref),
                (slot_hbm, slot_ref),
                (x_hbm, x_ref),
                (ct_hbm, ct_ref),
                (down_hbm, down_ref),
                (up_hbm, up_ref),
                (slot_hbm, slot_s),
            )
        )
    ]
    for copy in loads:
        copy.start()
    fetch(0).start()
    fetch(1).start()
    barrier = pltpu.get_barrier_semaphore()
    near = [device(*who) for who in sorted(meets)]
    for who in near:
        pl.semaphore_signal(barrier, inc=1, device_id=who, device_id_type=pl.DeviceIdType.MESH)

    for copy in loads[:3]:
        copy.wait()
    feats, span = slot_ref.shape[1], ids_ref.shape[0]
    each = slots * maxlen
    entry = lax.broadcasted_iota(jnp.int32, (span, feats), 0)
    hit = jnp.where(slot_ref[...] == entry // maxlen, 1.0, 0.0).astype(jnp.bfloat16)
    lens = jnp.dot(
        hit, len_ref[...].astype(jnp.float32).astype(jnp.bfloat16), preferred_element_type=jnp.float32
    )
    place = (lax.broadcasted_iota(jnp.int32, (span, batch), 0) % maxlen).astype(jnp.float32)
    idx = jnp.where(place < lens, ids_ref[...], rows)
    for o in range(owners):
        idx_ref[o] = idx[o * each : (o + 1) * each]

    def turn(src, dst):
        for n in range(depth // LANES):
            turned = src[:, n * LANES : (n + 1) * LANES].T
            begin, stop = n * LANES, (n + 1) * LANES
            while begin < stop:
                b, row = divmod(begin, high)
                size = min(high - row, stop - begin)
                dst[b, row : row + size] = turned[begin - n * LANES : begin - n * LANES + size]
                begin += size

    def peer(j):
        return (t // 2 + 1 - j // 2) % 2 * 2 + (t + (j + 1) // 2) % 2

    ids_out = [
        send(idx_ref.at[peer(j)], idx_in.at[j], idx_sem.at[0], idx_sem.at[1], (g, peer(j)))
        for j in range(owners - 1)
    ]
    ids_all = send(
        idx_in.at[pl.ds(0, owners - 1)],
        idx_in.at[pl.ds(0, owners - 1)],
        idx_sem.at[0],
        idx_sem.at[1],
        mate,
    )
    lent = pl.ds(pl.multiple_of((1 - core) * (high - half), 16), half)
    x_out, dz_out, low_out, dlow_out = (
        send(src, dst, mate_sem.at[0, n], mate_sem.at[1, n], mate)
        for n, (src, dst) in enumerate(
            (
                (xt.at[:, lent], x_in),
                (dzt.at[:, lent], dz_in),
                (low_ref, low_in),
                (dlow_ref, dlow_in),
            )
        )
    )
    for wide in (wide_even, wide_odd):
        wide[pl.ds(rows, 8), :] = jnp.zeros((8, width), jnp.float32)
    loads[3].wait()
    turn(x_ref, xt)
    pl.semaphore_wait(barrier, len(near))
    for copy in ids_out + [x_out]:
        copy.start()
    loads[4].wait()
    ct_ref[...] = (ct_ref[...].astype(jnp.float32) * x_ref[...].astype(jnp.float32)).astype(
        jnp.bfloat16
    )
    turn(ct_ref, dzt)
    dz_out.start()
    loads[5].wait()
    low_ref[...] = jnp.dot(
        x_ref[...], down_ref[...], preferred_element_type=jnp.float32
    ).astype(jnp.bfloat16)
    low_out.start()
    loads[6].wait()
    dlow = jnp.dot(
        up_ref[...], dzt[...].reshape(depth, batch), preferred_element_type=jnp.float32
    )
    dlow = dlow.astype(jnp.bfloat16).T
    swap = [n + 1 - 2 * (n % 2) for n in range(owners)]
    dlow_ref[...] = jnp.concatenate([dlow[:, n * cols : (n + 1) * cols] for n in swap], axis=1)
    dlow_out.start()

    wides = (wide_even, wide_odd)

    def widen(s, at):
        wides[s % 2][at, :] = stage[s % 2, at, :].astype(jnp.float32)

    fetch(0).wait()

    @pl.loop(0, rows // chunk)
    def _(c):
        widen(0, pl.ds(pl.multiple_of(c * chunk, chunk), chunk))

    ids_all.wait()
    idx_in[owners - 1] = idx_ref[t]
    got_ids = [
        pltpu.make_async_copy(
            idx_in.at[:, pl.ds(s * maxlen, maxlen)], idx_s.at[s], smem_sem.at[min(s, 2)]
        )
        for s in range(slots)
    ]
    for copy in got_ids:
        copy.start()
    dz_out.wait()
    low_out.wait()
    kept = pl.ds(pl.multiple_of(core * (high - half), 16), half)
    low_two = jnp.concatenate([low_ref[...], low_in[...]], axis=0)
    for b in range(groups):
        both = jnp.concatenate([dzt[b, kept], dz_in[b]], axis=1)
        rise[b] = jnp.dot(both, low_two, preferred_element_type=jnp.float32).astype(jnp.bfloat16)
    x_out.wait()
    dlow_out.wait()
    dlow_two = jnp.concatenate([dlow_ref[...], dlow_in[...]], axis=0)
    left = lax.broadcasted_iota(jnp.int32, (half, LANES), 1) < cols
    for b in range(groups):
        both = jnp.concatenate([xt[b, kept], x_in[b]], axis=1)
        down = jnp.dot(both, dlow_two, preferred_element_type=jnp.float32).astype(jnp.bfloat16)
        for y in range(2):
            u, d = rise[b, :, y * LANES : (y + 1) * LANES], down[:, y * LANES : (y + 1) * LANES]
            part[y, 0, b // 4, b // 2 % 2, b % 2] = jnp.where(left, u, d)
            part[y, 1, b // 4, b // 2 % 2, b % 2] = jnp.where(left, d, u)

    sizes = [n * half // 14 for _, _, n in PLAN]
    begins = [sum(sizes[:k]) for k in range(len(PLAN))]
    steps = [len(head) + 1 for head, _, _ in PLAN]

    def place_of(k, held):
        return tuple(held.get(d, slice(None)) for d in "ycvux") + (pl.ds(begins[k], sizes[k]),)

    def land(k, i):
        n = sum(steps[:k]) + i
        return landing[n], step_sem.at[k], step_sem.at[len(PLAN) + n]

    def exchange(k, i):
        head = PLAN[k][0]
        came, out_sem, in_sem = land(k, i)
        held = {d: at_axis[d] for d in head[:i]}
        held[head[i]] = 1 - at_axis[head[i]]
        return send(part.at[place_of(k, held)], came, out_sem, in_sem, device(head[i]))

    def last(k):
        final = PLAN[k][1]
        came, out_sem, in_sem = land(k, steps[k] - 1)
        ways = [(flip, turned) for turned in (False, True) for flip in flips(final)]
        copies = []
        for n, (flip, turned) in enumerate(ways + [("", True)]):
            held = {d: 1 - v if d in flip else v for d, v in at_axis.items()}
            held["c"] = 1 - core if turned else core
            copies.append(
                send(part.at[place_of(k, held)], came.at[n], out_sem, in_sem, device(flip, turned))
            )
        return copies

    def begin(k, i):
        if i < steps[k] - 1:
            exchange(k, i).start()
        else:
            for copy in last(k):
                copy.start()

    def take(k, i):
        head = PLAN[k][0]
        came, out_sem, in_sem = land(k, i)
        if i == steps[k] - 1:
            send(came, came, out_sem, in_sem, mate).wait()
            ways = came.shape[0] // 2
            other = pl.ds(pl.multiple_of((1 - core) * (high - half) + begins[k], 16), sizes[k])
            own = pl.ds(pl.multiple_of(core * (high - half) + begins[k], 16), sizes[k])
            mine = part[place_of(k, at_axis | {"c": core})].astype(jnp.float32)
            theirs = came[2 * ways].astype(jnp.float32)
            for n in range(ways):
                mine += came[n].astype(jnp.float32)
                theirs += came[ways + n].astype(jnp.float32)
            full[other, :] = theirs
            full[own, :] = mine
            return
        exchange(k, i).wait()
        held = {d: at_axis[d] for d in head[: i + 1]}
        free = [d for d in "ycvux" if d not in held]
        for pick in itertools.product(range(2), repeat=len(free)):
            at = place_of(k, held | dict(zip(free, pick)))
            part[at] = (part[at].astype(jnp.float32) + came[pick].astype(jnp.float32)).astype(
                jnp.bfloat16
            )
        begin(k, i + 1)

    for k in range(len(PLAN)):
        if k not in dict(LATE):
            begin(k, 0)

    def give(s, j):
        return send(
            pooled.at[j, s], got.at[t, s], pool_sem.at[0, j], pool_sem.at[1, j], (g, peer(j))
        )

    share = rows // owners
    for s in range(slots):
        if s < 2:
            got_ids[s].wait()
        elif s == 2:
            later = pl.ds(2, slots - 2)
            pltpu.make_async_copy(idx_s.at[later], idx_s.at[later], smem_sem.at[2]).wait()
        if s + 1 < slots:
            fetch(s + 1).wait()
        if s + 2 < slots:
            fetch(s + 2).start()
        wide = wides[s % 2]

        @pl.loop(0, owners)
        def _(j):
            if s + 1 < slots:
                widen(s + 1, pl.ds(pl.multiple_of(j * share, share), share))
            ids = [idx_s.at[s, j, k] for k in range(maxlen)]
            for u in range(batch):
                held = [wide[pl.ds(ids[k][u], 1), :] for k in range(maxlen)]
                while len(held) > 1:
                    held = [a + b for a, b in zip(held[::2], held[1::2])]
                acc[pl.ds(u, 1), :] = held[0]
            pooled[j, s] = acc[...].astype(jnp.bfloat16)

            @pl.when(j < owners - 1)
            def _():
                give(s, j).start()

            for n in range(owners):
                now = s * owners + n
                todo = [p for p in POLLS if p[0] == now]
                fresh = [k for k, p in LATE if p == now]
                if todo or fresh:

                    @pl.when(j == n)
                    def _():
                        for _, k, i in todo:
                            take(k, i)
                        for k in fresh:
                            begin(k, 0)

        got[t, s] = pooled[owners - 1, s]

    tail = [(k, i) for now, k, i in POLLS if now >= slots * owners]
    for n, (k, i) in enumerate(tail):
        if n == SORT:
            for j in range(owners - 1):
                send(
                    pooled.at[j], got.at[peer(j)], pool_sem.at[0, j], pool_sem.at[1, j], (g, peer(j))
                ).wait()
            loads[7].wait()
            for f in range(feats):
                s = slot_s[0, f]
                emb_ref[:, f * width : (f + 1) * width] = got[lax.div(s, slots), lax.rem(s, slots)]
        take(k, i)
    total = full[...].T
    out_ref[core] = total[:cols] * factor
    out_ref[1 - core] = total[cols:] * factor


def fused_step(
    next_ids, next_lengths, slot_of_table, tables, cross_input, cotangent, up_weight, down_weight, maxlen, factor
):
    groups, owners = lax.axis_size("grp"), lax.axis_size("tbl")
    slots, rows, width = tables.shape
    batch, depth = cross_input.shape
    rank = down_weight.shape[1]
    high = depth // groups
    half = (high // 2 + 15) // 16 * 16
    sems = pltpu.SemaphoreType.DMA
    bf16, f32 = jnp.bfloat16, jnp.float32
    in_hbm = pl.BlockSpec(memory_space=pltpu.HBM)
    idx_shape = (owners, next_ids.shape[1] // owners, batch)
    vmem = pl.BlockSpec(memory_space=pltpu.VMEM)
    landing = []
    for head, final, n in PLAN:
        rows_of = (n * half // 14, LANES)
        landing += [pltpu.VMEM((2,) * (4 - i) + rows_of, bf16) for i in range(len(head))]
        landing.append(pltpu.VMEM((2 * len(flips(final)) + 1,) + rows_of, bf16))
    return pl.pallas_call(
        functools.partial(step_kernel, maxlen, factor),
        out_shape=(
            pltpu.VMEM((batch, slot_of_table.shape[0] * width), bf16),
            pltpu.VMEM((2, rank // owners, high), f32),
        ),
        in_specs=[in_hbm] * 8,
        out_specs=(vmem, vmem),
        scratch_shapes=[
            pltpu.VMEM(next_ids.shape[::-1], jnp.int32),
            pltpu.VMEM(next_lengths.shape[::-1], jnp.int32),
            pltpu.VMEM((1, slot_of_table.shape[0]), jnp.int32),
            pltpu.SMEM((1, slot_of_table.shape[0]), jnp.int32),
            pltpu.VMEM(cross_input.shape, bf16),
            pltpu.VMEM(cotangent.shape, bf16),
            pltpu.VMEM(up_weight.shape, bf16),
            pltpu.VMEM(down_weight.shape, bf16),
            pltpu.VMEM((groups, high, batch), bf16),
            pltpu.VMEM((groups, high, batch), bf16),
            pltpu.VMEM((groups, half, batch), bf16),
            pltpu.VMEM((groups, half, batch), bf16),
            pltpu.VMEM((batch, rank), bf16),
            pltpu.VMEM((batch, rank), bf16),
            pltpu.VMEM((batch, rank), bf16),
            pltpu.VMEM((batch, rank), bf16),
            pltpu.VMEM(idx_shape, jnp.int32),
            pltpu.VMEM(idx_shape, jnp.int32),
            pltpu.SMEM((slots, owners, maxlen, batch), jnp.int32),
            pltpu.VMEM((groups, half, rank), bf16),
            pltpu.VMEM((2, 2, 2, 2, 2, half, LANES), bf16),
            pltpu.VMEM((high, LANES), f32),
            pltpu.VMEM((2, rows, width), bf16),
            pltpu.VMEM((rows + 8, width), f32),
            pltpu.VMEM((rows + 8, width), f32),
            pltpu.VMEM((batch, width), f32),
            pltpu.VMEM((owners, slots, batch, width), bf16),
            pltpu.VMEM((owners, slots, batch, width), bf16),
            sems((2,)),
            sems((3,)),
            sems((2,)),
            sems((2, 4)),
            sems((len(PLAN) + len(landing),)),
            sems((2, owners - 1)),
            sems((8,)),
        ]
        + landing,
        compiler_params=pltpu.CompilerParams(
            collective_id=0, has_side_effects=True, vmem_limit_bytes=48 << 20
        ),
        name="fused_step",
    )(
        *(
            pltpu.with_memory_space_constraint(a, pltpu.HBM)
            for a in (
                next_ids.T,
                next_lengths.T,
                slot_of_table[None, :],
                tables,
                cross_input,
                cotangent,
                up_weight,
                down_weight,
            )
        )
    )


def finish_kernel(emb_in, sum_in, emb_ref, grad_up_ref, grad_down_ref, sem):
    copies = [
        pltpu.make_async_copy(a, b, sem.at[n])
        for n, (a, b) in enumerate(
            ((emb_in, emb_ref), (sum_in.at[0], grad_up_ref), (sum_in.at[1], grad_down_ref))
        )
    ]
    for copy in copies:
        copy.start()
    for copy in copies:
        copy.wait()


def finish(emb, sums):
    in_hbm = pl.BlockSpec(memory_space=pltpu.HBM)
    any_space = pl.BlockSpec(memory_space=pl.ANY)
    return pl.pallas_call(
        finish_kernel,
        out_shape=(
            jax.ShapeDtypeStruct(emb.shape, emb.dtype),
            jax.ShapeDtypeStruct(sums.shape[1:], jnp.float32),
            jax.ShapeDtypeStruct(sums.shape[1:], jnp.float32),
        ),
        in_specs=[any_space, any_space],
        out_specs=(in_hbm, in_hbm, in_hbm),
        scratch_shapes=[pltpu.SemaphoreType.DMA((3,))],
        compiler_params=pltpu.CompilerParams(vmem_limit_bytes=1 << 20),
        name="finish",
    )(emb, sums)


def on_device(
    next_ids, next_lengths, slot_of_table, tables, cross_input, cotangent, up_weight, down_weight
):
    groups, owners = lax.axis_size("grp"), lax.axis_size("tbl")
    batch, depth = cross_input.shape
    rank = down_weight.shape[1]
    slots, rows, _ = tables.shape
    maxlen = next_ids.shape[1] // (slots * owners)
    fits = (
        owners == 4
        and groups == 8
        and depth % (16 * groups) == 0
        and depth % LANES == 0
        and depth // groups <= 448
        and depth // groups > 432 - 16
        and rank == 256
        and maxlen == 8
        and slots > 2
        and rows % 1024 == 0
        and batch == LANES
    )
    args = (
        next_ids,
        next_lengths,
        slot_of_table,
        tables,
        cross_input,
        cotangent,
        up_weight,
        down_weight,
    )
    if not fits:
        return plain(*args)
    factor = 1.0 / math.sqrt(batch * groups * owners)
    next_embedded, grad_up, grad_down = finish(*fused_step(*args, maxlen, factor))
    return next_embedded, grad_up, grad_down.T


def solution(mesh):
    return jax.shard_map(
        on_device,
        mesh=mesh,
        in_specs=(
            P(("grp", "tbl"), None),
            P(("grp", "tbl"), None),
            P(),
            P("tbl", None, None),
            P(("grp", "tbl"), None),
            P(("grp", "tbl"), None),
            P(),
            P(),
        ),
        out_specs=(P(("grp", "tbl"), None), P("tbl", "grp"), P("grp", "tbl")),
        check_vma=False,
    )
```

```python
import functools
import itertools
import math

import jax
import jax.numpy as jnp
from jax import lax
from jax.experimental import pallas as pl
from jax.experimental.pallas import tpu as pltpu
from jax.sharding import PartitionSpec as P

LANES = 128


def pool_kernel(maxlen, idx_ref, tab_ref, out_ref, stage, wide, acc, sem):
    owners, batch, _ = out_ref.shape
    slots, rows, width = tab_ref.shape
    per_line = LANES // maxlen
    lines = batch // per_line
    chunk = 256

    def fetch(s):
        return pltpu.make_async_copy(tab_ref.at[s], stage.at[s % 2], sem.at[s % 2])

    fetch(0).start()
    wide[pl.ds(rows, 8), :] = jnp.zeros((8, width), jnp.float32)
    for s in range(slots):
        if s + 1 < slots:
            fetch(s + 1).start()
        fetch(s).wait()

        @pl.loop(0, rows // chunk)
        def _(c):
            at = pl.ds(pl.multiple_of(c * chunk, chunk), chunk)
            wide[at, :] = stage[s % 2, at, :].astype(jnp.float32)

        @pl.loop(0, owners * lines)
        def _(g):
            src = g // lines
            line = s * lines + g % lines
            for u in range(per_line):
                got = [
                    wide[pl.ds(idx_ref[src, line, u * maxlen + k], 1), :] for k in range(maxlen)
                ]
                while len(got) > 1:
                    got = [a + b for a, b in zip(got[::2], got[1::2])] + (
                        [got[-1]] if len(got) % 2 else []
                    )
                acc[pl.ds(g * per_line + u, 1), :] = got[0]

        for o in range(owners):
            out_ref[o, :, s * width : (s + 1) * width] = acc[
                o * batch : (o + 1) * batch, :
            ].astype(jnp.bfloat16)


def pool(idx, tables, batch, maxlen):
    slots, rows, width = tables.shape
    owners = idx.shape[0]
    return pl.pallas_call(
        functools.partial(pool_kernel, maxlen),
        out_shape=jax.ShapeDtypeStruct((owners, batch, slots * width), jnp.bfloat16),
        in_specs=[
            pl.BlockSpec(memory_space=pltpu.SMEM),
            pl.BlockSpec(memory_space=pl.ANY),
        ],
        out_specs=pl.BlockSpec(memory_space=pltpu.VMEM),
        scratch_shapes=[
            pltpu.VMEM((2, rows, width), jnp.bfloat16),
            pltpu.VMEM((rows + 8, width), jnp.float32),
            pltpu.VMEM((owners * batch, width), jnp.float32),
            pltpu.SemaphoreType.DMA((2,)),
        ],
        compiler_params=pltpu.CompilerParams(vmem_limit_bytes=60 << 20),
        cost_estimate=pl.CostEstimate(
            flops=100_000_000, bytes_accessed=tables.size * 2, transcendentals=0
        ),
        name="pool",
    )(idx, tables)


def order_kernel(slot_ref, got_ref, out_ref):
    owners, batch, wide = got_ref.shape
    feats = slot_ref.shape[0]
    width = out_ref.shape[1] // feats
    slots = wide // width
    for f in range(feats):
        s = slot_ref[f]
        at = pl.ds(pl.multiple_of(lax.rem(s, slots) * width, width), width)
        out_ref[:, f * width : (f + 1) * width] = got_ref[lax.div(s, slots), :, at]


def order(slot_of_table, got, width):
    return pl.pallas_call(
        order_kernel,
        out_shape=jax.ShapeDtypeStruct(
            (got.shape[1], slot_of_table.shape[0] * width), jnp.bfloat16
        ),
        in_specs=[
            pl.BlockSpec(memory_space=pltpu.SMEM),
            pl.BlockSpec(memory_space=pltpu.VMEM),
        ],
        out_specs=pl.BlockSpec(memory_space=pltpu.VMEM),
        name="order",
    )(slot_of_table, got)


def bag_rows(next_ids, next_lengths, slot_of_table, slots, owners, rows):
    batch = next_ids.shape[0]
    slots_all = slots * owners
    maxlen = next_ids.shape[1] // slots_all
    hit = (slot_of_table[:, None] == lax.broadcasted_iota(jnp.int32, (1, slots_all), 1)).astype(
        jnp.int32
    )
    slot_lengths = jnp.sum(next_lengths[:, :, None] * hit[None, :, :], axis=1)
    keep = lax.broadcasted_iota(jnp.int32, (batch, slots_all, maxlen), 2) < slot_lengths[:, :, None]
    idx = jnp.where(keep, next_ids.reshape(batch, slots_all, maxlen), rows)
    return idx.transpose(1, 0, 2).reshape(owners, slots * batch * maxlen // LANES, LANES)


def plain(
    next_ids, next_lengths, slot_of_table, tables, cross_input, cotangent, up_weight, down_weight
):
    batch = next_ids.shape[0]
    owners = lax.axis_size("tbl")
    slots, rows, width = tables.shape
    maxlen = next_ids.shape[1] // (slots * owners)
    idx = bag_rows(next_ids, next_lengths, slot_of_table, slots, owners, rows)
    low = jnp.dot(cross_input, down_weight, preferred_element_type=jnp.float32).astype(jnp.bfloat16)
    dz = (cotangent.astype(jnp.float32) * cross_input.astype(jnp.float32)).astype(jnp.bfloat16)
    dlow = jnp.dot(dz, up_weight.T, preferred_element_type=jnp.float32).astype(jnp.bfloat16)
    total = batch * lax.axis_size("grp") * owners
    factor = 1.0 / math.sqrt(total)
    part_up = jnp.dot(low.T, dz, preferred_element_type=jnp.float32) * factor
    part_down = jnp.dot(cross_input.T, dlow, preferred_element_type=jnp.float32) * factor
    part_up, part_down = part_up.astype(jnp.bfloat16), part_down.astype(jnp.bfloat16)
    owner_up, owner_down = (
        lax.psum_scatter(part_up, "tbl", scatter_dimension=0, tiled=True).astype(jnp.float32),
        lax.psum_scatter(part_down, "tbl", scatter_dimension=1, tiled=True).astype(jnp.float32),
    )
    got_idx = lax.all_to_all(idx, "tbl", split_axis=0, concat_axis=0, tiled=True)
    pooled = pool(got_idx, tables, batch, maxlen)
    returned = lax.all_to_all(pooled, "tbl", split_axis=0, concat_axis=0, tiled=True)
    next_embedded = order(slot_of_table, returned, width)
    grad_up, grad_down = (
        lax.psum_scatter(owner_up, "grp", scatter_dimension=1, tiled=True),
        lax.psum_scatter(owner_down, "grp", scatter_dimension=0, tiled=True),
    )
    return (next_embedded, grad_up, grad_down)


PLAN = (("vyu", "x", 2), ("xu", "vy", 2), ("yxv", "u", 3), ("xuy", "v", 4), ("uv", "xy", 3))
POLLS = ((11, 3, 0), (12, 0, 0), (13, 4, 0), (15, 2, 0), (19, 1, 0), (20, 0, 1), (22, 2, 1), (22, 3, 1), (27, 0, 2), (27, 4, 1), (27, 1, 1), (28, 3, 2), (28, 2, 2), (28, 0, 3), (28, 2, 3), (28, 4, 2), (28, 1, 2), (28, 3, 3))
LATE = ((1, 10),)
SORT = 2


def flips(final):
    return ["".join(p) for n in range(1, len(final) + 1) for p in itertools.combinations(final, n)]


def step_kernel(
    maxlen,
    factor,
    ids_hbm,
    len_hbm,
    slot_hbm,
    tab_ref,
    x_hbm,
    ct_hbm,
    up_hbm,
    down_hbm,
    emb_ref,
    out_ref,
    ids_ref,
    len_ref,
    slot_ref,
    slot_s,
    x_ref,
    ct_ref,
    up_ref,
    down_ref,
    xt,
    dzt,
    x_in,
    dz_in,
    low_ref,
    dlow_ref,
    low_in,
    dlow_in,
    idx_ref,
    idx_in,
    idx_s,
    rise,
    part,
    full,
    stage,
    wide_even,
    wide_odd,
    acc,
    pooled,
    got,
    tab_sem,
    smem_sem,
    idx_sem,
    mate_sem,
    step_sem,
    pool_sem,
    load_sem,
    *landing,
):
    slots, rows, width = tab_ref.shape
    batch, depth = x_ref.shape
    rank = down_ref.shape[1]
    half = x_in.shape[1]
    owners, groups = 4, 8
    high = depth // groups
    cols = rank // owners
    chunk = 1024
    g, t = lax.axis_index("grp"), lax.axis_index("tbl")
    core = t % 2
    at_axis = {"y": t // 2, "v": g // 4, "u": g // 2 % 2, "x": g % 2}

    def device(flip, turned=False):
        at = {d: 1 - v if d in flip else v for d, v in at_axis.items()}
        c = 1 - core if turned else core
        return at["v"] * 4 + at["u"] * 2 + at["x"], at["y"] * 2 + c

    mate = device("", True)
    meets = {("y", False), ("y", True), ("", True)}
    for head, final, _ in PLAN:
        meets |= {(d, False) for d in head}
        meets |= {(flip, c) for flip in flips(final) for c in (False, True)}

    def fetch(s):
        return pltpu.make_async_copy(tab_ref.at[s], stage.at[s % 2], tab_sem.at[s % 2])

    def send(src, dst, out_sem, in_sem, who):
        return pltpu.make_async_remote_copy(
            src_ref=src,
            dst_ref=dst,
            send_sem=out_sem,
            recv_sem=in_sem,
            device_id=who,
            device_id_type=pl.DeviceIdType.MESH,
        )

    loads = [
        pltpu.make_async_copy(a, b, load_sem.at[n])
        for n, (a, b) in enumerate(
            (
                (ids_hbm, ids_ref),
                (len_hbm, len_ref),
                (slot_hbm, slot_ref),
                (x_hbm, x_ref),
                (ct_hbm, ct_ref),
                (down_hbm, down_ref),
                (up_hbm, up_ref),
                (slot_hbm, slot_s),
            )
        )
    ]
    for copy in loads:
        copy.start()
    fetch(0).start()
    fetch(1).start()
    barrier = pltpu.get_barrier_semaphore()
    near = [device(*who) for who in sorted(meets)]
    for who in near:
        pl.semaphore_signal(barrier, inc=1, device_id=who, device_id_type=pl.DeviceIdType.MESH)

    for copy in loads[:3]:
        copy.wait()
    feats, span = slot_ref.shape[1], ids_ref.shape[0]
    each = slots * maxlen
    entry = lax.broadcasted_iota(jnp.int32, (span, feats), 0)
    hit = jnp.where(slot_ref[...] == entry // maxlen, 1.0, 0.0).astype(jnp.bfloat16)
    lens = jnp.dot(
        hit, len_ref[...].astype(jnp.float32).astype(jnp.bfloat16), preferred_element_type=jnp.float32
    )
    place = (lax.broadcasted_iota(jnp.int32, (span, batch), 0) % maxlen).astype(jnp.float32)
    idx = jnp.where(place < lens, ids_ref[...], rows)
    for o in range(owners):
        idx_ref[o] = idx[o * each : (o + 1) * each]

    def turn(src, dst):
        for n in range(depth // LANES):
            turned = src[:, n * LANES : (n + 1) * LANES].T
            begin, stop = n * LANES, (n + 1) * LANES
            while begin < stop:
                b, row = divmod(begin, high)
                size = min(high - row, stop - begin)
                dst[b, row : row + size] = turned[begin - n * LANES : begin - n * LANES + size]
                begin += size

    def peer(j):
        return (t // 2 + 1 - j // 2) % 2 * 2 + (t + (j + 1) // 2) % 2

    ids_out = [
        send(idx_ref.at[peer(j)], idx_in.at[j], idx_sem.at[0], idx_sem.at[1], (g, peer(j)))
        for j in range(owners - 1)
    ]
    ids_all = send(
        idx_in.at[pl.ds(0, owners - 1)],
        idx_in.at[pl.ds(0, owners - 1)],
        idx_sem.at[0],
        idx_sem.at[1],
        mate,
    )
    lent = pl.ds(pl.multiple_of((1 - core) * (high - half), 16), half)
    x_out, dz_out, low_out, dlow_out = (
        send(src, dst, mate_sem.at[0, n], mate_sem.at[1, n], mate)
        for n, (src, dst) in enumerate(
            (
                (xt.at[:, lent], x_in),
                (dzt.at[:, lent], dz_in),
                (low_ref, low_in),
                (dlow_ref, dlow_in),
            )
        )
    )
    for wide in (wide_even, wide_odd):
        wide[pl.ds(rows, 8), :] = jnp.zeros((8, width), jnp.float32)
    loads[3].wait()
    turn(x_ref, xt)
    pl.semaphore_wait(barrier, len(near))
    for copy in ids_out + [x_out]:
        copy.start()
    loads[4].wait()
    ct_ref[...] = (ct_ref[...].astype(jnp.float32) * x_ref[...].astype(jnp.float32)).astype(
        jnp.bfloat16
    )
    turn(ct_ref, dzt)
    dz_out.start()
    loads[5].wait()
    low_ref[...] = jnp.dot(
        x_ref[...], down_ref[...], preferred_element_type=jnp.float32
    ).astype(jnp.bfloat16)
    low_out.start()
    loads[6].wait()
    dlow = jnp.dot(
        up_ref[...], dzt[...].reshape(depth, batch), preferred_element_type=jnp.float32
    )
    dlow = dlow.astype(jnp.bfloat16).T
    swap = [n + 1 - 2 * (n % 2) for n in range(owners)]
    dlow_ref[...] = jnp.concatenate([dlow[:, n * cols : (n + 1) * cols] for n in swap], axis=1)
    dlow_out.start()

    wides = (wide_even, wide_odd)

    def widen(s, at):
        wides[s % 2][at, :] = stage[s % 2, at, :].astype(jnp.float32)

    fetch(0).wait()

    @pl.loop(0, rows // chunk)
    def _(c):
        widen(0, pl.ds(pl.multiple_of(c * chunk, chunk), chunk))

    ids_all.wait()
    idx_in[owners - 1] = idx_ref[t]
    got_ids = [
        pltpu.make_async_copy(
            idx_in.at[:, pl.ds(s * maxlen, maxlen)], idx_s.at[s], smem_sem.at[min(s, 2)]
        )
        for s in range(slots)
    ]
    for copy in got_ids:
        copy.start()
    dz_out.wait()
    low_out.wait()
    kept = pl.ds(pl.multiple_of(core * (high - half), 16), half)
    low_two = jnp.concatenate([low_ref[...], low_in[...]], axis=0)
    for b in range(groups):
        both = jnp.concatenate([dzt[b, kept], dz_in[b]], axis=1)
        rise[b] = jnp.dot(both, low_two, preferred_element_type=jnp.float32).astype(jnp.bfloat16)
    x_out.wait()
    dlow_out.wait()
    dlow_two = jnp.concatenate([dlow_ref[...], dlow_in[...]], axis=0)
    left = lax.broadcasted_iota(jnp.int32, (half, LANES), 1) < cols
    for b in range(groups):
        both = jnp.concatenate([xt[b, kept], x_in[b]], axis=1)
        down = jnp.dot(both, dlow_two, preferred_element_type=jnp.float32).astype(jnp.bfloat16)
        for y in range(2):
            u, d = rise[b, :, y * LANES : (y + 1) * LANES], down[:, y * LANES : (y + 1) * LANES]
            part[y, 0, b // 4, b // 2 % 2, b % 2] = jnp.where(left, u, d)
            part[y, 1, b // 4, b // 2 % 2, b % 2] = jnp.where(left, d, u)

    sizes = [n * half // 14 for _, _, n in PLAN]
    begins = [sum(sizes[:k]) for k in range(len(PLAN))]
    steps = [len(head) + 1 for head, _, _ in PLAN]

    def place_of(k, held):
        return tuple(held.get(d, slice(None)) for d in "ycvux") + (pl.ds(begins[k], sizes[k]),)

    def land(k, i):
        n = sum(steps[:k]) + i
        return landing[n], step_sem.at[k], step_sem.at[len(PLAN) + n]

    def exchange(k, i):
        head = PLAN[k][0]
        came, out_sem, in_sem = land(k, i)
        held = {d: at_axis[d] for d in head[:i]}
        held[head[i]] = 1 - at_axis[head[i]]
        return send(part.at[place_of(k, held)], came, out_sem, in_sem, device(head[i]))

    def last(k):
        final = PLAN[k][1]
        came, out_sem, in_sem = land(k, steps[k] - 1)
        ways = [(flip, turned) for turned in (False, True) for flip in flips(final)]
        copies = []
        for n, (flip, turned) in enumerate(ways + [("", True)]):
            held = {d: 1 - v if d in flip else v for d, v in at_axis.items()}
            held["c"] = 1 - core if turned else core
            copies.append(
                send(part.at[place_of(k, held)], came.at[n], out_sem, in_sem, device(flip, turned))
            )
        return copies

    def begin(k, i):
        if i < steps[k] - 1:
            exchange(k, i).start()
        else:
            for copy in last(k):
                copy.start()

    def take(k, i):
        head = PLAN[k][0]
        came, out_sem, in_sem = land(k, i)
        if i == steps[k] - 1:
            send(came, came, out_sem, in_sem, mate).wait()
            ways = came.shape[0] // 2
            other = pl.ds(pl.multiple_of((1 - core) * (high - half) + begins[k], 16), sizes[k])
            own = pl.ds(pl.multiple_of(core * (high - half) + begins[k], 16), sizes[k])
            mine = part[place_of(k, at_axis | {"c": core})].astype(jnp.float32)
            theirs = came[2 * ways].astype(jnp.float32)
            for n in range(ways):
                mine += came[n].astype(jnp.float32)
                theirs += came[ways + n].astype(jnp.float32)
            full[other, :] = theirs
            full[own, :] = mine
            return
        exchange(k, i).wait()
        held = {d: at_axis[d] for d in head[: i + 1]}
        free = [d for d in "ycvux" if d not in held]
        for pick in itertools.product(range(2), repeat=len(free)):
            at = place_of(k, held | dict(zip(free, pick)))
            part[at] = (part[at].astype(jnp.float32) + came[pick].astype(jnp.float32)).astype(
                jnp.bfloat16
            )
        begin(k, i + 1)

    for k in range(len(PLAN)):
        if k not in dict(LATE):
            begin(k, 0)

    def give(s, j):
        return send(
            pooled.at[j, s], got.at[t, s], pool_sem.at[0, j], pool_sem.at[1, j], (g, peer(j))
        )

    share = rows // owners
    for s in range(slots):
        if s < 2:
            got_ids[s].wait()
        elif s == 2:
            later = pl.ds(2, slots - 2)
            pltpu.make_async_copy(idx_s.at[later], idx_s.at[later], smem_sem.at[2]).wait()
        if s + 1 < slots:
            fetch(s + 1).wait()
        if s + 2 < slots:
            fetch(s + 2).start()
        wide = wides[s % 2]

        @pl.loop(0, owners)
        def _(j):
            if s + 1 < slots:
                widen(s + 1, pl.ds(pl.multiple_of(j * share, share), share))
            ids = [idx_s.at[s, j, k] for k in range(maxlen)]
            for u in range(batch):
                held = [wide[pl.ds(ids[k][u], 1), :] for k in range(maxlen)]
                while len(held) > 1:
                    held = [a + b for a, b in zip(held[::2], held[1::2])]
                acc[pl.ds(u, 1), :] = held[0]
            pooled[j, s] = acc[...].astype(jnp.bfloat16)

            @pl.when(j < owners - 1)
            def _():
                give(s, j).start()

            for n in range(owners):
                now = s * owners + n
                todo = [p for p in POLLS if p[0] == now]
                fresh = [k for k, p in LATE if p == now]
                if todo or fresh:

                    @pl.when(j == n)
                    def _():
                        for _, k, i in todo:
                            take(k, i)
                        for k in fresh:
                            begin(k, 0)

        got[t, s] = pooled[owners - 1, s]

    tail = [(k, i) for now, k, i in POLLS if now >= slots * owners]
    for n, (k, i) in enumerate(tail):
        if n == SORT:
            for j in range(owners - 1):
                send(
                    pooled.at[j], got.at[peer(j)], pool_sem.at[0, j], pool_sem.at[1, j], (g, peer(j))
                ).wait()
            loads[7].wait()
            for f in range(feats):
                s = slot_s[0, f]
                emb_ref[:, f * width : (f + 1) * width] = got[lax.div(s, slots), lax.rem(s, slots)]
        take(k, i)
    total = full[...].T
    out_ref[core] = total[:cols] * factor
    out_ref[1 - core] = total[cols:] * factor


def fused_step(
    next_ids, next_lengths, slot_of_table, tables, cross_input, cotangent, up_weight, down_weight, maxlen, factor
):
    groups, owners = lax.axis_size("grp"), lax.axis_size("tbl")
    slots, rows, width = tables.shape
    batch, depth = cross_input.shape
    rank = down_weight.shape[1]
    high = depth // groups
    half = (high // 2 + 15) // 16 * 16
    sems = pltpu.SemaphoreType.DMA
    bf16, f32 = jnp.bfloat16, jnp.float32
    in_hbm = pl.BlockSpec(memory_space=pltpu.HBM)
    idx_shape = (owners, next_ids.shape[1] // owners, batch)
    vmem = pl.BlockSpec(memory_space=pltpu.VMEM)
    landing = []
    for head, final, n in PLAN:
        rows_of = (n * half // 14, LANES)
        landing += [pltpu.VMEM((2,) * (4 - i) + rows_of, bf16) for i in range(len(head))]
        landing.append(pltpu.VMEM((2 * len(flips(final)) + 1,) + rows_of, bf16))
    return pl.pallas_call(
        functools.partial(step_kernel, maxlen, factor),
        out_shape=(
            pltpu.VMEM((batch, slot_of_table.shape[0] * width), bf16),
            pltpu.VMEM((2, rank // owners, high), f32),
        ),
        in_specs=[in_hbm] * 8,
        out_specs=(vmem, vmem),
        scratch_shapes=[
            pltpu.VMEM(next_ids.shape[::-1], jnp.int32),
            pltpu.VMEM(next_lengths.shape[::-1], jnp.int32),
            pltpu.VMEM((1, slot_of_table.shape[0]), jnp.int32),
            pltpu.SMEM((1, slot_of_table.shape[0]), jnp.int32),
            pltpu.VMEM(cross_input.shape, bf16),
            pltpu.VMEM(cotangent.shape, bf16),
            pltpu.VMEM(up_weight.shape, bf16),
            pltpu.VMEM(down_weight.shape, bf16),
            pltpu.VMEM((groups, high, batch), bf16),
            pltpu.VMEM((groups, high, batch), bf16),
            pltpu.VMEM((groups, half, batch), bf16),
            pltpu.VMEM((groups, half, batch), bf16),
            pltpu.VMEM((batch, rank), bf16),
            pltpu.VMEM((batch, rank), bf16),
            pltpu.VMEM((batch, rank), bf16),
            pltpu.VMEM((batch, rank), bf16),
            pltpu.VMEM(idx_shape, jnp.int32),
            pltpu.VMEM(idx_shape, jnp.int32),
            pltpu.SMEM((slots, owners, maxlen, batch), jnp.int32),
            pltpu.VMEM((groups, half, rank), bf16),
            pltpu.VMEM((2, 2, 2, 2, 2, half, LANES), bf16),
            pltpu.VMEM((high, LANES), f32),
            pltpu.VMEM((2, rows, width), bf16),
            pltpu.VMEM((rows + 8, width), f32),
            pltpu.VMEM((rows + 8, width), f32),
            pltpu.VMEM((batch, width), f32),
            pltpu.VMEM((owners, slots, batch, width), bf16),
            pltpu.VMEM((owners, slots, batch, width), bf16),
            sems((2,)),
            sems((3,)),
            sems((2,)),
            sems((2, 4)),
            sems((len(PLAN) + len(landing),)),
            sems((2, owners - 1)),
            sems((8,)),
        ]
        + landing,
        compiler_params=pltpu.CompilerParams(
            collective_id=0, has_side_effects=True, vmem_limit_bytes=48 << 20
        ),
        name="fused_step",
    )(
        *(
            pltpu.with_memory_space_constraint(a, pltpu.HBM)
            for a in (
                next_ids.T,
                next_lengths.T,
                slot_of_table[None, :],
                tables,
                cross_input,
                cotangent,
                up_weight,
                down_weight,
            )
        )
    )


def finish_kernel(emb_in, sum_in, emb_ref, grad_up_ref, grad_down_ref, sem):
    copies = [
        pltpu.make_async_copy(a, b, sem.at[n])
        for n, (a, b) in enumerate(
            ((emb_in, emb_ref), (sum_in.at[0], grad_up_ref), (sum_in.at[1], grad_down_ref))
        )
    ]
    for copy in copies:
        copy.start()
    for copy in copies:
        copy.wait()


def finish(emb, sums):
    in_hbm = pl.BlockSpec(memory_space=pltpu.HBM)
    any_space = pl.BlockSpec(memory_space=pl.ANY)
    return pl.pallas_call(
        finish_kernel,
        out_shape=(
            jax.ShapeDtypeStruct(emb.shape, emb.dtype),
            jax.ShapeDtypeStruct(sums.shape[1:], jnp.float32),
            jax.ShapeDtypeStruct(sums.shape[1:], jnp.float32),
        ),
        in_specs=[any_space, any_space],
        out_specs=(in_hbm, in_hbm, in_hbm),
        scratch_shapes=[pltpu.SemaphoreType.DMA((3,))],
        compiler_params=pltpu.CompilerParams(vmem_limit_bytes=1 << 20),
        name="finish",
    )(emb, sums)


def on_device(
    next_ids, next_lengths, slot_of_table, tables, cross_input, cotangent, up_weight, down_weight
):
    groups, owners = lax.axis_size("grp"), lax.axis_size("tbl")
    batch, depth = cross_input.shape
    rank = down_weight.shape[1]
    slots, rows, _ = tables.shape
    maxlen = next_ids.shape[1] // (slots * owners)
    fits = (
        owners == 4
        and groups == 8
        and depth % (16 * groups) == 0
        and depth % LANES == 0
        and depth // groups <= 448
        and depth // groups > 432 - 16
        and rank == 256
        and maxlen == 8
        and slots > 2
        and rows % 1024 == 0
        and batch == LANES
    )
    args = (
        next_ids,
        next_lengths,
        slot_of_table,
        tables,
        cross_input,
        cotangent,
        up_weight,
        down_weight,
    )
    if not fits:
        return plain(*args)
    factor = 1.0 / math.sqrt(batch * groups * owners)
    next_embedded, grad_up, grad_down = finish(*fused_step(*args, maxlen, factor))
    return next_embedded, grad_up, grad_down.T


def solution(mesh):
    return jax.shard_map(
        on_device,
        mesh=mesh,
        in_specs=(
            P(("grp", "tbl"), None),
            P(("grp", "tbl"), None),
            P(),
            P("tbl", None, None),
            P(("grp", "tbl"), None),
            P(("grp", "tbl"), None),
            P(),
            P(),
        ),
        out_specs=(P(("grp", "tbl"), None), P("tbl", "grp"), P("grp", "tbl")),
        check_vma=False,
    )
```
